32 devices in a mesh: gx: 4 (over x, core), gy: 4 (over z), gz: 2 (over y).
Axes of the slice: x: 2, y: 2, z: 4, core: 2. Of those that a mesh axis runs over, the one named last changes fastest.
Arguments:
- velocity: float32 [3, 64, 128, 256], P(None, 'gx', 'gy', 'gz'), may hold values from -4 to 4
- plane_early: float32 [3, 128, 256], P(None, 'gy', 'gx'), may hold values from -4 to 4
- plane_late: float32 [3, 128, 256], P(None, 'gy', 'gx'), may hold values from -4 to 4
- blend: float32 [1], replicated, may hold values from 0 to 1
Outputs:
- advanced: float32 [3, 64, 128, 256], P(None, 'gx', 'gy', 'gz')
The draws below stay inside these ranges and needn't reach their ends.
All inputs are finite; a program needn't handle non-finite values.
Results may differ from the reference program's by a relative error of at most 0.00002.
Values sent between devices are 32-bit elements; how exact they have to be, the bound alone decides.
A program may use at most 64 MiB of HBM per device.

```python
import jax
import jax.numpy as jnp

STEPS = 4
NX = 64
NY = 128
NZ = 256


def steps_of(stream_key, extent, pieces, smallest, top_value):
    factor_of, own = 1.0, jax.random.fold_in(stream_key, 6)
    for position, shards_of in pieces:
        heights = jnp.exp(jax.random.uniform(jax.random.fold_in(own, position), (shards_of,), jnp.float32, smallest / len(pieces), top_value / len(pieces)))
        factor_of = factor_of * jnp.repeat(heights, extent[position] // shards_of).reshape([-1 if axis == position else 1 for axis in range(len(extent))])
    return factor_of


def normal_values(key, extent, spread, bound, cuts=(), held_as=jnp.bfloat16):
    array = spread * jax.random.normal(key, extent, jnp.float32)
    if cuts:
        array = array * steps_of(key, extent, cuts, -0.22, 0.18)
    return jnp.clip(array, -bound, bound).astype(held_as)


def setup_inputs(seed: int = 0) -> dict:
    arg_keys = jax.random.split(jax.random.key(seed), 5)
    return {
        "velocity": normal_values(arg_keys[0], (3, NX, NY, NZ), 1.0, 4.0, ((1, 4), (2, 4), (3, 2)), jnp.float32),
        "plane_early": normal_values(arg_keys[1], (3, NY, NZ), 1.0, 4.0, ((1, 4), (2, 4)), jnp.float32),
        "plane_late": normal_values(arg_keys[2], (3, NY, NZ), 1.0, 4.0, ((1, 4), (2, 4)), jnp.float32),
        "blend": jnp.clip(jax.random.uniform(arg_keys[3], (1,), jnp.float32, 0.0, 1.0), 0.0, 1.0),
    }


courant = 0.08


def advect(padded):
    center = padded[:, 1:-1, 1:-1, 1:-1]
    stream_u = center[0:1]
    span_v = center[1:2]
    vert_w = center[2:3]
    back_x = center - padded[:, :-2, 1:-1, 1:-1]
    ahead_x = padded[:, 2:, 1:-1, 1:-1] - center
    back_y = center - padded[:, 1:-1, :-2, 1:-1]
    ahead_y = padded[:, 1:-1, 2:, 1:-1] - center
    back_z = center - padded[:, 1:-1, 1:-1, :-2]
    ahead_z = padded[:, 1:-1, 1:-1, 2:] - center
    tendency = (jnp.maximum(stream_u, 0.0) * back_x + jnp.minimum(stream_u, 0.0) * ahead_x) \
        + (jnp.maximum(span_v, 0.0) * back_y + jnp.minimum(span_v, 0.0) * ahead_y) \
        + (jnp.maximum(vert_w, 0.0) * back_z + jnp.minimum(vert_w, 0.0) * ahead_z)
    return center - courant * tendency


def reference(velocity, plane_early, plane_late, blend):
    weight = blend[0]
    inflow = (1.0 - weight) * plane_early + weight * plane_late
    inflow_span = jnp.concatenate([inflow[:, -1:], inflow, inflow[:, :1]], axis=1)
    current = velocity
    for substep in range(STEPS):
        padded = jnp.concatenate([current[:, :, -1:], current, current[:, :, :1]], axis=2)
        empty_slab = jnp.zeros_like(inflow_span)[:, None]
        padded = jnp.concatenate([inflow_span[:, None], padded, empty_slab], axis=1)
        padded = jnp.pad(padded, ((0, 0), (0, 0), (0, 0), (1, 1)))
        current = advect(padded)
    return current
```

```python
import functools

import jax
import jax.numpy as jnp
from jax import lax
from jax.experimental import pallas as pl
from jax.experimental.pallas import tpu as pltpu
from jax.sharding import PartitionSpec as P

STEPS = 4
COURANT = 0.08
DEPTH = STEPS
TILE = 8
TOP = 8
GROUP = 4 * DEPTH

MESH = pl.DeviceIdType.MESH


def kernel(sizes, vel_hbm, early_hbm, late_hbm, blend_ref, out_ref,
           cur, y_halo, strip_send, strip_recv, feed_send, feed_recv, inflow, fixed,
           early, late, load_sem, ss, rs, fs, fr):
    nx, ny, nz = sizes
    comps, cells_x, cells_y, cells_z = vel_hbm.shape
    share = nx // nz
    piece = early_hbm.shape[2]
    gx, gy, gz = (lax.axis_index(name) for name in ("gx", "gy", "gz"))
    own = pl.ds(TOP, cells_y)
    first = DEPTH
    after = DEPTH + cells_x
    strips = cells_x + 2 * DEPTH
    groups = cells_z // GROUP
    rings = (cells_x + 2 * DEPTH) // groups
    half = GROUP // 2
    row_blocks = [TOP + TILE * b for b in range(cells_y // TILE)]
    low_rows, high_rows = TOP - DEPTH, TOP + cells_y - DEPTH

    load_v = pltpu.make_async_copy(
        vel_hbm, cur.at[0, :, pl.ds(first, cells_x), own, :], load_sem.at[0])
    load_e = pltpu.make_async_copy(early_hbm, early, load_sem.at[1])
    load_l = pltpu.make_async_copy(late_hbm, late, load_sem.at[2])
    load_e.start()
    load_l.start()
    load_v.start()

    has_left, has_right = gx > 0, gx < nx - 1
    always = gx >= 0
    others = {-1: has_left, 0: always, 1: has_right}

    def target(dx, dy, dz):
        where = {}
        if dx:
            where["gx"] = gx + dx
        if dy:
            where["gy"] = lax.rem(gy + dy + ny, ny)
        if dz:
            where["gz"] = 1 - gz
        return where

    needed = lambda k: (k // share == gz) | (share - gz == k)
    feeds = (gx != 0) & needed(gx)

    barrier = pltpu.get_barrier_semaphore()
    expected = jnp.int32(0)
    for dx in (0, -1, 1):
        for dy in (-1, 1, 0):
            for dz in (0, 1):
                if (dx, dy, dz) == (0, 0, 0):
                    continue

                @pl.when(others[dx])
                def _(where=target(dx, dy, dz)):
                    pl.semaphore_signal(barrier, 1, device_id=where, device_id_type=MESH)
                expected = expected + jnp.where(others[dx], 1, 0)
    for k in range(2, nx):
        for dy in (-1, 1, 0):
            @pl.when((gx == 0) & needed(k))
            def _(k=k, dy=dy):
                pl.semaphore_signal(
                    barrier, 1, device_id={"gx": k, "gy": lax.rem(gy + dy + ny, ny)},
                    device_id_type=MESH)
    expected = expected + jnp.where((gx >= 2) & feeds, 3, 0)

    count = [0]

    def message(dx, dy, dz, src, dst):
        k = count[0]
        count[0] += 1
        return others[dx], others[-dx], pltpu.make_async_remote_copy(
            src_ref=src, dst_ref=dst, send_sem=ss.at[k], recv_sem=rs.at[k],
            device_id=target(dx, dy, dz), device_id_type=MESH)

    def rows_out(dy, depth, base):
        return pl.ds(base + cells_y - depth if dy > 0 else base, depth)

    def rows_in(dy, depth, base, size):
        return pl.ds(base - depth if dy > 0 else base + size, depth)

    inside = pl.ds(first, cells_x)
    reach = DEPTH - 1
    y_messages = {}
    for dy in (1, -1):
        side = 0 if dy > 0 else 1
        into = lambda depth: rows_in(dy, depth, TILE if dy > 0 else 0, 0)
        y_messages[side] = [
            message(0, dy, 0, cur.at[0, :, inside, rows_out(dy, DEPTH, TOP), :],
                    y_halo.at[side, :, inside, into(DEPTH), :])]
        for dx in (1, -1):
            src = pl.ds(after - reach if dx > 0 else first, reach)
            dst = pl.ds(first - reach if dx > 0 else after, reach)
            y_messages[side].append(
                message(dx, dy, 0, cur.at[0, :, src, rows_out(dy, reach, TOP), :],
                        y_halo.at[side, :, dst, into(reach), :]))
        y_messages[side].append(
            message(0, dy, 1, strip_send.at[:, 0, rows_out(dy, reach, 0), :],
                    strip_recv.at[:, 0, rows_in(dy, reach, TOP, cells_y), :]))
        for dx in (1, -1):
            y_messages[side].append(
                message(dx, dy, 1, strip_send.at[:, 1, rows_out(dy, reach - 1, 0), :],
                        strip_recv.at[:, 1 if dx > 0 else 2,
                                      rows_in(dy, reach - 1, TOP, cells_y), :]))
    x_messages = [
        message(1, 0, 0, cur.at[0, :, pl.ds(after - DEPTH, DEPTH), own, :],
                cur.at[0, :, pl.ds(0, DEPTH), own, :]),
        message(-1, 0, 0, cur.at[0, :, pl.ds(first, DEPTH), own, :],
                cur.at[0, :, pl.ds(after, DEPTH), own, :])]
    z_messages = [message(0, 0, 1, strip_send.at[:, 0], strip_recv.at[:, 0, own, :])]
    for dx in (1, -1):
        z_messages.append(
            message(dx, 0, 1, strip_send.at[:, 1],
                    strip_recv.at[:, 1 if dx > 0 else 2, own, :]))

    feed_rows = {0: (pl.ds(0, cells_y), own),
                 1: (rows_out(1, reach, 0), rows_in(1, reach, TOP, cells_y)),
                 -1: (rows_out(-1, reach, 0), rows_in(-1, reach, TOP, cells_y))}

    def feed(k, dy):
        src, dst = feed_rows[dy]
        where = {"gx": 0}
        if dy:
            where["gy"] = lax.rem(gy + dy + ny, ny)
        return pltpu.make_async_remote_copy(
            src_ref=feed_send.at[:, src, :], dst_ref=feed_recv.at[k, :, dst, :],
            send_sem=fs.at[k, dy + 1], recv_sem=fr.at[k, dy + 1],
            device_id=where, device_id_type=MESH)

    def feeding(k, dy):
        if k == 0:
            return (gx == 0) & needed(0) if dy else None
        return (gx == k) & needed(k)

    def start(messages):
        for sends, _, copy in messages:
            pl.when(sends)(copy.start)

    def arrived(messages):
        for _, receives, copy in messages:
            pl.when(receives)(copy.wait_recv)

    lane = lax.broadcasted_iota(jnp.int32, (TILE, cells_z), 1)
    group = lane // GROUP
    mine = lax.rem(lane, GROUP) // half == gz
    held = ((lane >= jnp.where(gx == 0, cells_z - GROUP, cells_z))
            | (lane < jnp.where(gx == nx - 1, GROUP, 0)))
    edge = lax.rem(lane + gz * (cells_z - DEPTH), cells_z) >= cells_z - DEPTH
    up_z = jnp.where(lane == 0, 0.0, COURANT)
    down_z = jnp.where(lane == cells_z - 1, 0.0, -COURANT)

    load_e.wait()
    load_l.wait()
    weight = blend_ref[0]
    mixed = (1.0 - weight) * early[...] + weight * late[...]
    feed_send[...] = jnp.concatenate([mixed] * share, axis=2)

    load_v.wait()

    def turn(j):
        return (GROUP * j + half) % cells_z

    def pack(ring, c, rows):
        acc = None
        for j in range(groups):
            x = groups * ring + j
            p = first + x if x < cells_x + DEPTH else x - cells_x - DEPTH
            turned = pltpu.roll(cur[0, c, p, rows, :], turn(j), 1)
            acc = turned if acc is None else jnp.where(group == j, turned, acc)
        return acc

    for c in range(comps):
        for r in row_blocks:
            packed = [pack(ring, c, pl.ds(r, TILE)) for ring in range(rings - 1)]
            for ring in range(rings - 1):
                cur[0, c, strips + ring, pl.ds(r, TILE), :] = packed[ring]
            strip_send[c, 0, pl.ds(r - TOP, TILE), :] = jnp.where(
                mine, packed[0], pltpu.roll(packed[1], cells_z - half, 1))
            strip_send[c, 1, pl.ds(r - TOP, TILE), :] = jnp.where(
                group < groups // 2, packed[0], packed[-1])

    pl.semaphore_wait(barrier, expected)

    @pl.when(gy == 0)
    def _():
        start(y_messages[1])
        start(y_messages[0])

    @pl.when(gy != 0)
    def _():
        start(y_messages[0])
        start(y_messages[1])

    start(x_messages)
    start(z_messages)
    for k in range(nx):
        for dy in (0, 1, -1):
            sends = feeding(k, dy)
            if sends is not None:
                pl.when(sends)(feed(k, dy).start)

    @pl.when((gx == 0) & needed(0))
    def _():
        feed_recv[0, :, own, :] = feed_send[...]

    def advance(q, behind, ahead, inner):
        scaled = [COURANT * q[d] for d in range(3)]
        sizes_of = [jnp.abs(s) for s in scaled]
        keep = 1.0 - sizes_of[0] - sizes_of[1] - sizes_of[2]
        if inner:
            sizes_of[2] = jnp.maximum(up_z * q[2], down_z * q[2])
        positive = [q[d] > 0.0 for d in range(3)]
        result = []
        for c in range(comps):
            total = keep * q[c]
            for d in range(3):
                total += sizes_of[d] * jnp.where(positive[d], behind[d][c], ahead[d][c])
            result.append(total)
        return result

    def main(t, p, r):
        def load(dp, dr):
            return [cur[t, c, p + dp, pl.ds(r + dr, TILE), :] for c in range(comps)]

        q = load(0, 0)
        behind = [load(-1, 0), load(0, -1), [pltpu.roll(v, 1, 1) for v in q]]
        ahead = [load(1, 0), load(0, 1), [pltpu.roll(v, cells_z - 1, 1) for v in q]]
        return advance(q, behind, ahead, True)

    def merged(x, r, values):
        back = lax.rem(2 * cells_z - GROUP * lax.rem(x, groups) - half, cells_z)
        ring = strips + x // groups
        return [jnp.where(edge, pltpu.roll(cur[STEPS, c, ring, pl.ds(r, TILE), :], back, 1),
                          values[c]) for c in range(comps)]

    def planes(low, high, body, unroll):
        if low >= high:
            return
        if high - low <= unroll:
            for x in range(low, high):
                body(x)
            return

        def step(x, carry):
            body(x)
            return carry

        lax.fori_loop(low, high, step, 0, unroll=unroll)

    def block(t, low, high, unroll=2):
        def body(x):
            for r in row_blocks:
                values = main(t, x + first, r)
                if t == STEPS - 1:
                    values = merged(x, r, values)
                    for c in range(comps):
                        out_ref[c, x, pl.ds(r - TOP, TILE), :] = values[c]
                else:
                    for c in range(comps):
                        cur[t + 1, c, x + first, pl.ds(r, TILE), :] = values[c]

        planes(low, high, body, unroll)

    def window(t, low, high, side, unroll=4):
        r = high_rows if side else low_rows

        def body(x):
            values = main(t, x + first, r)
            if t == STEPS - 1:
                values = merged(x, r, values)
                for c in range(comps):
                    if side:
                        out_ref[c, x, cells_y - DEPTH:cells_y, :] = values[c][:DEPTH]
                    else:
                        out_ref[c, x, 0:DEPTH, :] = values[c][TILE - DEPTH:]
            else:
                for c in range(comps):
                    cur[t + 1, c, x + first, pl.ds(r, TILE), :] = values[c]

        planes(low, high, body, unroll)

    def around(t, r):
        def load(k, dr):
            return [cur[t, c, strips + k, pl.ds(r + dr, TILE), :] for c in range(comps)]

        ring = [load(k, 0) for k in range(rings)]
        last = t == STEPS - 1
        for k in range(rings - 1 if last else rings):
            q, before, later = ring[k], ring[k - 1], ring[(k + 1) % rings]
            behind = [
                [pltpu.roll(jnp.where(group == groups - 1, before[c], q[c]), GROUP, 1)
                 for c in range(comps)],
                load(k, -1), [pltpu.roll(v, 1, 1) for v in q]]
            ahead = [
                [pltpu.roll(jnp.where(group == 0, later[c], q[c]), cells_z - GROUP, 1)
                 for c in range(comps)],
                load(k, 1), [pltpu.roll(v, cells_z - 1, 1) for v in q]]
            values = advance(q, behind, ahead, False)
            for c in range(comps):
                value = values[c]
                if k == rings - 1:
                    value = jnp.where(held, fixed[c, pl.ds(r, TILE), :], value)
                cur[t + 1, c, strips + k, pl.ds(r, TILE), :] = value

    def assemble(r):
        rows = pl.ds(r, TILE)
        for c in range(comps):
            near = strip_recv[c, 0, rows, :]
            far = jnp.where(group < groups // 2, strip_recv[c, 2, rows, :],
                            strip_recv[c, 1, rows, :])
            theirs = [near, pltpu.roll(near, half, 1), far]
            for ring in range(rings):
                if ring < rings - 1 and r in row_blocks:
                    ours = cur[0, c, strips + ring, rows, :]
                else:
                    ours = pack(ring, c, rows)
                value = jnp.where(mine, ours, theirs[ring])
                if ring == rings - 1:
                    value = jnp.where(held, fixed[c, rows, :], value)
                cur[0, c, strips + ring, rows, :] = value

    def boundary(r, size):
        @pl.when(gx == 0)
        def _():
            for c in range(comps):
                for b in range(0, size, TILE):
                    rows = pl.ds(r + b, TILE)
                    plane = feed_recv[gz * share, c, rows, :]
                    for k in range(1, share):
                        plane = jnp.where(lane // piece == k,
                                          feed_recv[gz * share + k, c, rows, :], plane)
                    inflow[c, rows, :] = plane
                    beyond = feed_recv[share - gz, c, rows, :]
                    there = turn(groups - 1)
                    window_values = jnp.where(mine, pltpu.roll(plane, there, 1),
                                              pltpu.roll(beyond, there, 1))
                    fixed[c, rows, :] = jnp.where(group == groups - 1, window_values, 0.0)
                    for t in range(STEPS):
                        cur[t, c, first - 1, rows, :] = plane

        @pl.when(gx != 0)
        def _():
            for c in range(comps):
                for b in range(0, size, TILE):
                    fixed[c, pl.ds(r + b, TILE), :] = jnp.zeros((TILE, cells_z), jnp.float32)

        @pl.when(gx == nx - 1)
        def _():
            for c in range(comps):
                for b in range(0, size, TILE):
                    for t in range(STEPS):
                        cur[t, c, after, pl.ds(r + b, TILE), :] = jnp.zeros(
                            (TILE, cells_z), jnp.float32)

    def feed_arrived(dy):
        for k in range(nx):
            if k == 0 and dy == 0:
                continue
            pl.when((gx == 0) & needed(k))(feed(k, dy).wait_recv)

    for t in range(STEPS - 1):
        block(t, t + 1, cells_x - 1 - t)
    arrived(x_messages)
    feed_arrived(0)
    boundary(TOP, cells_y)
    for t in range(STEPS - 1):
        beyond = STEPS - 1 - t

        @pl.when(has_left)
        def _(t=t, beyond=beyond):
            block(t, -beyond, 0)

        @pl.when(has_right)
        def _(t=t, beyond=beyond):
            block(t, cells_x, cells_x + beyond)

        block(t, 0, t + 1)
        block(t, cells_x - 1 - t, cells_x)
    arrived(z_messages)

    for r in row_blocks:
        assemble(r)
    for t in range(STEPS):
        for r in row_blocks:
            around(t, r)
    block(STEPS - 1, 0, cells_x)

    def finish(side):
        r = high_rows if side else low_rows
        arrived(y_messages[side])
        feed_arrived(-1 if side else 1)
        halo = pl.ds(TOP + cells_y, DEPTH) if side else pl.ds(TOP - DEPTH, DEPTH)
        held_rows = pl.ds(0, DEPTH) if side else pl.ds(TILE - DEPTH, DEPTH)

        def copy_rows(x):
            for c in range(comps):
                cur[0, c, x + first, halo, :] = y_halo[side, c, x + first, held_rows, :]

        planes(-reach, cells_x + reach, copy_rows, 2)
        boundary(r, TILE)
        assemble(r)
        for t in range(STEPS):
            beyond = STEPS - 1 - t
            if beyond:
                @pl.when(has_left)
                def _():
                    window(t, -beyond, 0, side)

                @pl.when(has_right)
                def _():
                    window(t, cells_x, cells_x + beyond, side)
            around(t, r)
            window(t, 0, cells_x, side)

    @pl.when(gy == 0)
    def _():
        finish(1)
        finish(0)

    @pl.when(gy != 0)
    def _():
        finish(0)
        finish(1)

    for sends, _, copy in y_messages[0] + y_messages[1] + x_messages + z_messages:
        pl.when(sends)(copy.wait_send)
    for k in range(nx):
        for dy in (0, 1, -1):
            sends = feeding(k, dy)
            if sends is not None:
                pl.when(sends)(feed(k, dy).wait_send)


def local(sizes, velocity, plane_early, plane_late, blend):
    comps, cells_x, cells_y, cells_z = velocity.shape
    nx, ny, nz = sizes
    groups = cells_z // GROUP
    assert nz == 2 and ny > 2 and nx % nz == 0 and cells_z == 128
    assert cells_x == 2 * groups and 2 * DEPTH == groups and cells_y % TILE == 0
    dma = pltpu.SemaphoreType.DMA
    padded = cells_y + 2 * TOP
    planes = cells_x + 2 * DEPTH
    return pl.pallas_call(
        functools.partial(kernel, sizes),
        out_shape=pltpu.VMEM(velocity.shape, velocity.dtype),
        in_specs=[pl.BlockSpec(memory_space=pl.ANY)] * 3
        + [pl.BlockSpec(memory_space=pltpu.SMEM)],
        out_specs=pl.BlockSpec(memory_space=pltpu.VMEM),
        scratch_shapes=[
            pltpu.VMEM((STEPS + 1, comps, planes + 3, padded, cells_z), jnp.float32),
            pltpu.VMEM((2, comps, planes, TILE, cells_z), jnp.float32),
            pltpu.VMEM((comps, 2, cells_y, cells_z), jnp.float32),
            pltpu.VMEM((comps, 3, padded, cells_z), jnp.float32),
            pltpu.VMEM((comps, cells_y, cells_z), jnp.float32),
            pltpu.VMEM((nx, comps, padded, cells_z), jnp.float32),
            pltpu.VMEM((comps, padded, cells_z), jnp.float32),
            pltpu.VMEM((comps, padded, cells_z), jnp.float32),
            pltpu.VMEM(plane_early.shape, jnp.float32),
            pltpu.VMEM(plane_late.shape, jnp.float32),
            dma((3,)), dma((17,)), dma((17,)), dma((nx, 3)), dma((nx, 3)),
        ],
        compiler_params=pltpu.CompilerParams(collective_id=0, has_side_effects=True),
        name="advect_substeps",
    )(velocity, plane_early, plane_late, blend)


def solution(mesh):
    sizes = tuple(mesh.shape[name] for name in ("gx", "gy", "gz"))
    return jax.shard_map(
        functools.partial(local, sizes),
        mesh=mesh,
        in_specs=(P(None, "gx", "gy", "gz"), P(None, "gy", "gx"), P(None, "gy", "gx"), P()),
        out_specs=P(None, "gx", "gy", "gz"),
        check_vma=False,
    )
```

```python
import functools

import jax
import jax.numpy as jnp
from jax import lax
from jax.experimental import pallas as pl
from jax.experimental.pallas import tpu as pltpu
from jax.sharding import PartitionSpec as P

STEPS = 4
COURANT = 0.08
DEPTH = STEPS
TILE = 8
TOP = 8
GROUP = 4 * DEPTH

MESH = pl.DeviceIdType.MESH
scope = jax.named_scope


def kernel(sizes, vel_hbm, early_hbm, late_hbm, blend_ref, out_ref,
           cur, strip_send, strip_recv, feed_send, feed_recv, inflow, fixed,
           early, late, late_sem, load_sem, ss, rs, fs, fr):
    nx, ny, nz = sizes
    comps, cells_x, cells_y, cells_z = vel_hbm.shape
    share = nx // nz
    piece = early_hbm.shape[2]
    gx, gy, gz = (lax.axis_index(name) for name in ("gx", "gy", "gz"))
    own = pl.ds(TOP, cells_y)
    first = DEPTH
    after = DEPTH + cells_x
    strips = cells_x + 2 * DEPTH
    groups = cells_z // GROUP
    rings = (cells_x + 2 * DEPTH) // groups
    half = GROUP // 2
    row_blocks = [TOP + TILE * b for b in range(cells_y // TILE)]
    low_rows, high_rows = TOP - DEPTH, TOP + cells_y - DEPTH

    load_v = pltpu.make_async_copy(
        vel_hbm, cur.at[0, :, pl.ds(first, cells_x), own, :], load_sem.at[0])
    load_e = pltpu.make_async_copy(early_hbm, early, load_sem.at[1])
    load_l = pltpu.make_async_copy(late_hbm, late, load_sem.at[2])
    load_e.start()
    load_l.start()
    load_v.start()

    has_left, has_right = gx > 0, gx < nx - 1
    always = gx >= 0
    others = {-1: has_left, 0: always, 1: has_right}
    bottom, top = gy == 0, gy == ny - 1

    def spanwise(dy):
        return lax.rem(gy + dy + ny, ny)

    def target(dx, dy, dz):
        where = {}
        if dx:
            where["gx"] = gx + dx
        if dy:
            where["gy"] = spanwise(dy)
        if dz:
            where["gz"] = 1 - gz
        return where

    def needed(k):
        return (k // share == gz) | (share - gz == k)

    feeds = (gx != 0) & needed(gx)

    barrier = pltpu.get_barrier_semaphore()
    expected = jnp.int32(0)
    late_expected = jnp.int32(0)
    late_greetings = []

    def greet(semaphore, condition, where):
        @pl.when(condition)
        def _():
            pl.semaphore_signal(semaphore, 1, device_id=where, device_id_type=MESH)

    for dy in (-1, 1, 0):
        for dx in (0, -1, 1):
            for dz in (0, 1):
                if (dx, dy, dz) == (0, 0, 0):
                    continue
                there, where = others[dx], target(dx, dy, dz)
                one = jnp.where(there, 1, 0)
                if dy == 1:
                    greet(barrier, there & ~top, where)
                    late_greetings.append((there & top, where))
                else:
                    greet(barrier, there, where)
                if dy == -1:
                    expected = expected + jnp.where(bottom, 0, one)
                    late_expected = late_expected + one
                else:
                    expected = expected + one
    for k in range(2, nx):
        takes = (gx == 0) & needed(k)
        for dy in (-1, 1, 0):
            where = {"gx": k, "gy": spanwise(dy)}
            if dy == 1:
                greet(barrier, takes & ~top, where)
                late_greetings.append((takes & top, where))
            else:
                greet(barrier, takes, where)
        greet(barrier, (gx == k) & needed(k) & bottom, {"gx": 0, "gy": spanwise(-1)})
        expected = expected + jnp.where(takes & top, 1, 0)
    gives = (gx >= 2) & feeds
    expected = expected + jnp.where(gives, jnp.where(bottom, 2, 3), 0)
    late_expected = late_expected + jnp.where(gives, 1, 0)

    count = [0]

    def message(dx, dy, dz, src, dst):
        k = count[0]
        count[0] += 1
        return others[dx], others[-dx], pltpu.make_async_remote_copy(
            src_ref=src, dst_ref=dst, send_sem=ss.at[k], recv_sem=rs.at[k],
            device_id=target(dx, dy, dz), device_id_type=MESH)

    def rows_out(dy, depth, base):
        return pl.ds(base + cells_y - depth if dy > 0 else base, depth)

    def rows_in(dy, depth):
        return pl.ds(TOP - depth if dy > 0 else TOP + cells_y, depth)

    inside = pl.ds(first, cells_x)
    reach = DEPTH - 1
    y_main, y_strips = {}, {}
    for dy in (1, -1):
        y_main[dy] = [
            message(0, dy, 0, cur.at[0, :, inside, rows_out(dy, DEPTH, TOP), :],
                    cur.at[0, :, inside, rows_in(dy, DEPTH), :])]
        for dx in (1, -1):
            src = pl.ds(after - reach if dx > 0 else first, reach)
            dst = pl.ds(first - reach if dx > 0 else after, reach)
            y_main[dy].append(
                message(dx, dy, 0, cur.at[0, :, src, rows_out(dy, reach, TOP), :],
                        cur.at[0, :, dst, rows_in(dy, reach), :]))
        y_strips[dy] = [
            message(0, dy, 1, strip_send.at[:, 0, rows_out(dy, reach, 0), :],
                    strip_recv.at[:, 0, rows_in(dy, reach), :])]
        for dx in (1, -1):
            y_strips[dy].append(
                message(dx, dy, 1, strip_send.at[:, 1, rows_out(dy, reach - 1, 0), :],
                        strip_recv.at[:, 1 if dx > 0 else 2, rows_in(dy, reach - 1), :]))
    x_messages = [
        message(1, 0, 0, cur.at[0, :, pl.ds(after - DEPTH, DEPTH), own, :],
                cur.at[0, :, pl.ds(0, DEPTH), own, :]),
        message(-1, 0, 0, cur.at[0, :, pl.ds(first, DEPTH), own, :],
                cur.at[0, :, pl.ds(after, DEPTH), own, :])]
    z_messages = [message(0, 0, 1, strip_send.at[:, 0], strip_recv.at[:, 0, own, :])]
    for dx in (1, -1):
        z_messages.append(
            message(dx, 0, 1, strip_send.at[:, 1],
                    strip_recv.at[:, 1 if dx > 0 else 2, own, :]))

    def feed(k, dy):
        where = {"gx": 0}
        if dy:
            where["gy"] = spanwise(dy)
        src = rows_out(dy, reach, 0) if dy else pl.ds(0, cells_y)
        dst = rows_in(dy, reach) if dy else own
        return pltpu.make_async_remote_copy(
            src_ref=feed_send.at[:, src, :], dst_ref=feed_recv.at[k, :, dst, :],
            send_sem=fs.at[k, dy + 1], recv_sem=fr.at[k, dy + 1],
            device_id=where, device_id_type=MESH)

    def start_feed(dy):
        for k in range(nx):
            if k or dy:
                pl.when((gx == k) & needed(k))(feed(k, dy).start)

    def feed_arrived(dy):
        for k in range(nx):
            if k or dy:
                pl.when((gx == 0) & needed(k))(feed(k, dy).wait_recv)

    def start(messages):
        for sends, _, copy in messages:
            pl.when(sends)(copy.start)

    def arrived(messages):
        for _, receives, copy in messages:
            pl.when(receives)(copy.wait_recv)

    lane = lax.broadcasted_iota(jnp.int32, (TILE, cells_z), 1)
    group = lane // GROUP
    mine = lax.rem(lane, GROUP) // half == gz
    held = ((lane >= jnp.where(gx == 0, cells_z - GROUP, cells_z))
            | (lane < jnp.where(gx == nx - 1, GROUP, 0)))
    is_first = lane >= jnp.where(gx == 0, 0, cells_z)
    is_last = lane >= jnp.where(gx == nx - 1, 0, cells_z)
    edge = lax.rem(lane + gz * (cells_z - DEPTH), cells_z) >= cells_z - DEPTH
    up_z = jnp.where(lane == 0, 0.0, COURANT)
    down_z = jnp.where(lane == cells_z - 1, 0.0, -COURANT)

    with scope("load_el"):
        load_e.wait()
        load_l.wait()
    weight = blend_ref[0]
    mixed = (1.0 - weight) * early[...] + weight * late[...]
    feed_send[...] = jnp.concatenate([mixed] * share, axis=2)

    with scope("load_v"):
        load_v.wait()
    with scope("barrier"):
        pl.semaphore_wait(barrier, expected)
    with scope("send"):
        start(y_main[1])
        pl.when(~bottom)(lambda: start(y_main[-1]))
        start_feed(0)
        start(x_messages)
        for condition, where in late_greetings:
            greet(late_sem, condition, where)

    def turn(j):
        return (GROUP * j + half) % cells_z

    def pack(ring, c, rows):
        acc = None
        for j in range(groups):
            x = groups * ring + j
            p = first + x if x < cells_x + DEPTH else x - cells_x - DEPTH
            turned = pltpu.roll(cur[0, c, p, rows, :], turn(j), 1)
            acc = turned if acc is None else jnp.where(group == j, turned, acc)
        return acc

    with scope("pack"):
        for r in row_blocks:
            for c in range(comps):
                packed = [pack(ring, c, pl.ds(r, TILE)) for ring in range(rings - 1)]
                for ring in range(rings - 1):
                    cur[0, c, strips + ring, pl.ds(r, TILE), :] = packed[ring]
                strip_send[c, 0, pl.ds(r - TOP, TILE), :] = jnp.where(
                    mine, packed[0], pltpu.roll(packed[1], cells_z - half, 1))
                strip_send[c, 1, pl.ds(r - TOP, TILE), :] = jnp.where(
                    group < groups // 2, packed[0], packed[-1])

    with scope("send2"):
        start(y_strips[1])
        start(z_messages)
        start_feed(1)

        @pl.when(~bottom)
        def _():
            start(y_strips[-1])
            start_feed(-1)

    @pl.when((gx == 0) & needed(0))
    def _():
        feed_recv[0, :, own, :] = feed_send[...]

    def advance(q, behind, ahead, inner):
        scaled = [COURANT * q[d] for d in range(3)]
        weights = [jnp.abs(s) for s in scaled]
        keep = 1.0 - weights[0] - weights[1] - weights[2]
        if inner:
            weights[2] = jnp.maximum(up_z * q[2], down_z * q[2])
        positive = [q[d] > 0.0 for d in range(3)]
        result = []
        for c in range(comps):
            total = keep * q[c]
            for d in range(3):
                total += weights[d] * jnp.where(positive[d], behind[d][c], ahead[d][c])
            result.append(total)
        return result

    def shifted(t, p, r, dr, q):
        rows = r + dr
        if t == 0 and r in row_blocks and (rows < TOP or rows + TILE > TOP + cells_y):
            return [pltpu.roll(v, 1 if dr < 0 else TILE - 1, 0) for v in q]
        return [cur[t, c, p, pl.ds(rows, TILE), :] for c in range(comps)]

    def main(t, p, r):
        q, left, right = ([cur[t, c, p + dp, pl.ds(r, TILE), :] for c in range(comps)]
                          for dp in (0, -1, 1))
        behind = [left, shifted(t, p, r, -1, q), [pltpu.roll(v, 1, 1) for v in q]]
        ahead = [right, shifted(t, p, r, 1, q), [pltpu.roll(v, cells_z - 1, 1) for v in q]]
        return advance(q, behind, ahead, True)

    def merged(x, r, values):
        back = lax.rem(2 * cells_z - GROUP * lax.rem(x, groups) - half, cells_z)
        ring = strips + x // groups
        return [jnp.where(edge, pltpu.roll(cur[STEPS, c, ring, pl.ds(r, TILE), :], back, 1),
                          values[c]) for c in range(comps)]

    def plane(t, x, rows):
        for r in rows:
            values = main(t, x + first, r)
            if t < STEPS - 1:
                if isinstance(x, int) and x == -1:
                    values = [jnp.where(is_first, inflow[c, pl.ds(r, TILE), :], values[c])
                              for c in range(comps)]
                if isinstance(x, int) and x == cells_x:
                    values = [jnp.where(is_last, 0.0, v) for v in values]
                for c in range(comps):
                    cur[t + 1, c, x + first, pl.ds(r, TILE), :] = values[c]
                continue
            values = merged(x, r, values)
            for c in range(comps):
                if r == low_rows:
                    out_ref[c, x, 0:DEPTH, :] = values[c][TILE - DEPTH:]
                elif r == high_rows:
                    out_ref[c, x, cells_y - DEPTH:cells_y, :] = values[c][:DEPTH]
                else:
                    out_ref[c, x, pl.ds(r - TOP, TILE), :] = values[c]

    def planes(t, low, high, rows, unroll=None):
        cuts = sorted({low, high} | {k for k in (-1, 0, cells_x, cells_x + 1)
                                     if low < k < high})
        for begin, end in zip(cuts[:-1], cuts[1:]):
            if end - begin == 1:
                plane(t, begin, rows)
                continue

            def step(x, carry):
                plane(t, x, rows)
                return carry

            lax.fori_loop(begin, end, step, 0, unroll=unroll or end - begin)

    def around(t, r):
        ring = [[cur[t, c, strips + k, pl.ds(r, TILE), :] for c in range(comps)]
                for k in range(rings)]
        last = t == STEPS - 1

        def load(k, dr):
            return [cur[t, c, strips + k, pl.ds(r + dr, TILE), :] for c in range(comps)]

        for k in range(rings - 1 if last else rings):
            q, before, later = ring[k], ring[k - 1], ring[(k + 1) % rings]
            behind = [
                [pltpu.roll(jnp.where(group == groups - 1, before[c], q[c]), GROUP, 1)
                 for c in range(comps)],
                load(k, -1), [pltpu.roll(v, 1, 1) for v in q]]
            ahead = [
                [pltpu.roll(jnp.where(group == 0, later[c], q[c]), cells_z - GROUP, 1)
                 for c in range(comps)],
                load(k, 1), [pltpu.roll(v, cells_z - 1, 1) for v in q]]
            values = advance(q, behind, ahead, False)
            for c in range(comps):
                value = values[c]
                if k == rings - 1:
                    value = jnp.where(held, fixed[c, pl.ds(r, TILE), :], value)
                cur[t + 1, c, strips + k, pl.ds(r, TILE), :] = value

    def assemble(r):
        rows = pl.ds(r, TILE)
        for c in range(comps):
            near = strip_recv[c, 0, rows, :]
            far = jnp.where(group < groups // 2, strip_recv[c, 2, rows, :],
                            strip_recv[c, 1, rows, :])
            theirs = [near, pltpu.roll(near, half, 1), far]
            for ring in range(rings):
                if ring < rings - 1 and r in row_blocks:
                    ours = cur[0, c, strips + ring, rows, :]
                else:
                    ours = pack(ring, c, rows)
                value = jnp.where(mine, ours, theirs[ring])
                if ring == rings - 1:
                    value = jnp.where(held, fixed[c, rows, :], value)
                cur[0, c, strips + ring, rows, :] = value

    def ghosts(r):
        rows = pl.ds(r, TILE)
        for c in range(comps):
            values = feed_recv[gz * share, c, rows, :]
            for k in range(1, share):
                values = jnp.where(lane // piece == k,
                                   feed_recv[gz * share + k, c, rows, :], values)
            inflow[c, rows, :] = values
            beyond = feed_recv[share - gz, c, rows, :]
            there = turn(groups - 1)
            there_values = jnp.where(mine, pltpu.roll(values, there, 1),
                                     pltpu.roll(beyond, there, 1))
            fixed[c, rows, :] = jnp.where(is_first & (group == groups - 1), there_values, 0.0)
            cur[0, c, first - 1, rows, :] = jnp.where(
                is_first, values, cur[0, c, first - 1, rows, :])
            cur[0, c, after, rows, :] = jnp.where(is_last, 0.0, cur[0, c, after, rows, :])

    for t in range(STEPS - 1):
        with scope("A1_%d" % t):
            planes(t, t + 1, cells_x - 1 - t, row_blocks)

    @pl.when(bottom)
    def _():
        with scope("late"):
            pl.semaphore_wait(late_sem, late_expected)
        start(y_main[-1])
        start(y_strips[-1])
        start_feed(-1)

    with scope("x_wait"):
        arrived(x_messages)
    with scope("feed_wait"):
        feed_arrived(0)
    with scope("A2"):
        for r in row_blocks:
            ghosts(r)
        for t in range(STEPS - 1):
            beyond = STEPS - 1 - t
            planes(t, -beyond, t + 1, row_blocks)
            planes(t, cells_x - 1 - t, cells_x + beyond, row_blocks)
    with scope("z_wait"):
        arrived(z_messages)
    with scope("around"):
        for r in row_blocks:
            assemble(r)
        for t in range(STEPS):
            for r in row_blocks:
                around(t, r)
    with scope("final"):
        planes(STEPS - 1, 0, cells_x, row_blocks)

    def finish(dy):
        r = low_rows if dy > 0 else high_rows
        with scope("y_wait%d" % dy):
            arrived(y_main[dy])
            arrived(y_strips[dy])
            feed_arrived(dy)
        with scope("win%d" % dy):
            ghosts(r)
            assemble(r)
            for t in range(STEPS):
                beyond = STEPS - 1 - t
                around(t, r)
                planes(t, -beyond, cells_x + beyond, [r])

    @pl.when(bottom)
    def _():
        finish(-1)
        finish(1)

    @pl.when(~bottom)
    def _():
        finish(1)
        finish(-1)

    with scope("drain"):
        for dy in (1, -1):
            for sends, _, copy in y_main[dy] + y_strips[dy]:
                pl.when(sends)(copy.wait_send)
        for sends, _, copy in x_messages + z_messages:
            pl.when(sends)(copy.wait_send)
        for k in range(nx):
            for dy in (0, 1, -1):
                if k or dy:
                    pl.when((gx == k) & needed(k))(feed(k, dy).wait_send)


def local(sizes, velocity, plane_early, plane_late, blend):
    comps, cells_x, cells_y, cells_z = velocity.shape
    nx, ny, nz = sizes
    groups = cells_z // GROUP
    assert nz == 2 and ny > 2 and nx % nz == 0 and cells_z == 128
    assert cells_x == 2 * groups and 2 * DEPTH == groups and cells_y % TILE == 0
    dma = pltpu.SemaphoreType.DMA
    padded = cells_y + 2 * TOP
    planes = cells_x + 2 * DEPTH
    return pl.pallas_call(
        functools.partial(kernel, sizes),
        out_shape=pltpu.VMEM(velocity.shape, velocity.dtype),
        in_specs=[pl.BlockSpec(memory_space=pl.ANY)] * 3
        + [pl.BlockSpec(memory_space=pltpu.SMEM)],
        out_specs=pl.BlockSpec(memory_space=pltpu.VMEM),
        scratch_shapes=[
            pltpu.VMEM((STEPS + 1, comps, planes + 3, padded, cells_z), jnp.float32),
            pltpu.VMEM((comps, 2, cells_y, cells_z), jnp.float32),
            pltpu.VMEM((comps, 3, padded, cells_z), jnp.float32),
            pltpu.VMEM((comps, cells_y, cells_z), jnp.float32),
            pltpu.VMEM((nx, comps, padded, cells_z), jnp.float32),
            pltpu.VMEM((comps, padded, cells_z), jnp.float32),
            pltpu.VMEM((comps, padded, cells_z), jnp.float32),
            pltpu.VMEM(plane_early.shape, jnp.float32),
            pltpu.VMEM(plane_late.shape, jnp.float32),
            pltpu.SemaphoreType.REGULAR,
            dma((3,)), dma((17,)), dma((17,)), dma((nx, 3)), dma((nx, 3)),
        ],
        compiler_params=pltpu.CompilerParams(collective_id=0, has_side_effects=True),
        name="advect_substeps",
    )(velocity, plane_early, plane_late, blend)


def solution(mesh):
    sizes = tuple(mesh.shape[name] for name in ("gx", "gy", "gz"))
    return jax.shard_map(
        functools.partial(local, sizes),
        mesh=mesh,
        in_specs=(P(None, "gx", "gy", "gz"), P(None, "gy", "gx"), P(None, "gy", "gx"), P()),
        out_specs=P(None, "gx", "gy", "gz"),
        check_vma=False,
    )
```

```python
import functools

import jax
import jax.numpy as jnp
from jax import lax
from jax.experimental import pallas as pl
from jax.experimental.pallas import tpu as pltpu
from jax.sharding import PartitionSpec as P

STEPS = 4
COURANT = 0.08
DEPTH = STEPS
TILE = 8
TOP = 8
GROUP = 4 * DEPTH

MESH = pl.DeviceIdType.MESH
scope = jax.named_scope


def kernel(sizes, vel_hbm, early_hbm, late_hbm, blend_ref, out_ref,
           cur, strip_send, strip_recv, feed_send, feed_recv, inflow, fixed,
           early, late, tally, late_sem, load_sem, send_sem, recv_sem):
    nx, ny, nz = sizes
    comps, cells_x, cells_y, cells_z = vel_hbm.shape
    share = nx // nz
    piece = early_hbm.shape[2]
    gx, gy, gz = (lax.axis_index(name) for name in ("gx", "gy", "gz"))
    own = pl.ds(TOP, cells_y)
    first = DEPTH
    after = DEPTH + cells_x
    strips = cells_x + 2 * DEPTH
    groups = cells_z // GROUP
    rings = (cells_x + 2 * DEPTH) // groups
    half = GROUP // 2
    row_blocks = [TOP + TILE * b for b in range(cells_y // TILE)]
    low_rows, high_rows = TOP - DEPTH, TOP + cells_y - DEPTH

    load_v = pltpu.make_async_copy(
        vel_hbm, cur.at[0, :, pl.ds(first, cells_x), own, :], load_sem.at[0])
    load_e = pltpu.make_async_copy(early_hbm, early, load_sem.at[1])
    load_l = pltpu.make_async_copy(late_hbm, late, load_sem.at[2])
    load_e.start()
    load_l.start()
    load_v.start()

    has_left, has_right = gx > 0, gx < nx - 1
    always = gx >= 0
    others = {-1: has_left, 0: always, 1: has_right}
    bottom, top = gy == 0, gy == ny - 1

    def spanwise(dy):
        return lax.rem(gy + dy + ny, ny)

    def target(dx, dy, dz):
        where = {}
        if dx:
            where["gx"] = gx + dx
        if dy:
            where["gy"] = spanwise(dy)
        if dz:
            where["gz"] = 1 - gz
        return where

    def needed(k):
        return (k // share == gz) | (share - gz == k)

    feeds = (gx != 0) & needed(gx)

    def gain(dx, dy, dz):
        step = lax.div(gx + dx + 2, 2) - lax.div(gx + 2, 2)
        if dy:
            step = step + spanwise(dy) - gy
        return step + 1 - 2 * gz if dz else step

    barrier = pltpu.get_barrier_semaphore()
    NEAR, FAR = 0, 1
    expected = jnp.int32(0)
    late_expected = [jnp.int32(0), jnp.int32(0)]
    late_greetings = []
    soon, far = {}, {}

    def greet(semaphore, condition, where):
        @pl.when(condition)
        def _():
            pl.semaphore_signal(semaphore, 1, device_id=where, device_id_type=MESH)

    def await_greetings(semaphore, number):
        @pl.when(number > 0)
        def _():
            pl.semaphore_wait(semaphore, number)

    for dy in (-1, 1, 0):
        for dx in (0, -1, 1):
            for dz in (0, 1):
                place = (dx, dy, dz)
                if place == (0, 0, 0):
                    continue
                there, where, later = others[dx], target(*place), gain(*place)
                greet(barrier, there & (later >= 0), where)
                beyond = top if dy == 1 else gy < 0
                late_greetings.append((NEAR, there & (later < 0) & ~beyond, where))
                if dy == 1:
                    late_greetings.append((FAR, there & (later < 0) & beyond, where))
                soon[place] = later <= 0
                far[place] = (later > 0) & bottom if dy == -1 else gy < 0
                expected = expected + jnp.where(there & soon[place], 1, 0)
                late_expected[NEAR] = late_expected[NEAR] + jnp.where(
                    there & ~soon[place] & ~far[place], 1, 0)
                late_expected[FAR] = late_expected[FAR] + jnp.where(there & far[place], 1, 0)
    for k in range(2, nx):
        takes = (gx == 0) & needed(k)
        for dy in (-1, 1, 0):
            where = {"gx": k, "gy": spanwise(dy)}
            if dy == 1:
                greet(barrier, takes & ~top, where)
                late_greetings.append((FAR, takes & top, where))
            else:
                greet(barrier, takes, where)
        greet(barrier, (gx == k) & needed(k) & bottom, {"gx": 0, "gy": spanwise(-1)})
        expected = expected + jnp.where(takes & top, 1, 0)
    gives = (gx >= 2) & feeds
    expected = expected + jnp.where(gives, jnp.where(bottom, 2, 3), 0)
    late_expected[FAR] = late_expected[FAR] + jnp.where(gives & bottom, 1, 0)

    Y_UP, Y_DOWN, X, Z, FEED = range(5)
    y_group = {1: Y_UP, -1: Y_DOWN}
    volume = {}

    def rows_of(ref):
        rows = 1
        for extent in ref.shape[:-1]:
            rows *= extent
        return rows

    def message(group, dx, dy, dz, src, dst):
        volume[group, dx] = volume.get((group, dx), 0) + rows_of(src)
        return (dx, dy, dz), pltpu.make_async_remote_copy(
            src_ref=src, dst_ref=dst, send_sem=send_sem.at[0], recv_sem=recv_sem.at[group],
            device_id=target(dx, dy, dz), device_id_type=MESH)

    def settle(semaphore, rows):
        part = tally.at[pl.ds(0, rows)]
        pltpu.make_async_copy(part, part, semaphore).wait()

    at_left, at_right = gx == 0, gx == nx - 1

    def settle_by_place(semaphore, from_left, middle, from_right, extra_left=0):
        pl.when(at_left)(lambda: settle(semaphore, middle + from_right + extra_left))
        pl.when(at_right)(lambda: settle(semaphore, middle + from_left))
        pl.when(~at_left & ~at_right)(
            lambda: settle(semaphore, middle + from_left + from_right))

    def rows_out(dy, depth, base):
        return pl.ds(base + cells_y - depth if dy > 0 else base, depth)

    def rows_in(dy, depth):
        return pl.ds(TOP - depth if dy > 0 else TOP + cells_y, depth)

    inside = pl.ds(first, cells_x)
    reach = DEPTH - 1
    y_main, y_strips = {}, {}
    for dy in (1, -1):
        g = y_group[dy]
        y_main[dy] = []
        for dx in (1, -1):
            for d in range(1, DEPTH):
                src = after - d if dx > 0 else first + d - 1
                dst = first - d if dx > 0 else after + d - 1
                y_main[dy].append(
                    message(g, dx, dy, 0, cur.at[0, :, src, rows_out(dy, DEPTH - d, TOP), :],
                            cur.at[0, :, dst, rows_in(dy, DEPTH - d), :]))
        y_main[dy].append(
            message(g, 0, dy, 0, cur.at[0, :, inside, rows_out(dy, DEPTH, TOP), :],
                    cur.at[0, :, inside, rows_in(dy, DEPTH), :]))
        y_strips[dy] = [
            message(g, 0, dy, 1, strip_send.at[pl.ds(0, comps), rows_out(dy, reach, 0), :],
                    strip_recv.at[pl.ds(0, comps), rows_in(dy, reach), :])]
        for dx in (1, -1):
            slot = comps if dx > 0 else comps + 1
            y_strips[dy].append(
                message(g, dx, dy, 1, strip_send.at[slot, rows_out(dy, reach - 1, 0), :],
                        strip_recv.at[slot, rows_in(dy, reach - 1), :]))
    x_messages = [
        message(X, 1, 0, 0, cur.at[0, :, pl.ds(after - DEPTH, DEPTH), own, :],
                cur.at[0, :, pl.ds(0, DEPTH), own, :]),
        message(X, -1, 0, 0, cur.at[0, :, pl.ds(first, DEPTH), own, :],
                cur.at[0, :, pl.ds(after, DEPTH), own, :])]
    z_messages = [message(Z, 0, 0, 1, strip_send.at[pl.ds(0, comps)],
                          strip_recv.at[pl.ds(0, comps), own, :])]
    for dx in (1, -1):
        slot = comps if dx > 0 else comps + 1
        z_messages.append(
            message(Z, dx, 0, 1, strip_send.at[slot], strip_recv.at[slot, own, :]))

    def feed(k, dy):
        where = {"gx": 0}
        if dy:
            where["gy"] = spanwise(dy)
        src = rows_out(dy, reach, 0) if dy else pl.ds(0, cells_y)
        dst = rows_in(dy, reach) if dy else own
        return pltpu.make_async_remote_copy(
            src_ref=feed_send.at[:, src, :], dst_ref=feed_recv.at[k, :, dst, :],
            send_sem=send_sem.at[1], recv_sem=recv_sem.at[y_group[dy] if dy else FEED],
            device_id=where, device_id_type=MESH)

    def start_feed(dy, condition, ks=None):
        for k in ks or range(nx):
            if k or dy:
                pl.when((gx == k) & needed(k) & condition)(feed(k, dy).start)

    def pieces(z, dy):
        return [k for k in range(nx)
                if (k or dy) and (k // share == z or share - z == k)]

    def start(messages, phase, condition=None):
        for place, copy in messages:
            late = ~soon[place] & ~far[place]
            when = others[place[0]] & (soon[place], late, far[place])[phase]
            pl.when(when if condition is None else when & condition)(copy.start)

    def group_arrived(g, extra_left=0):
        settle_by_place(recv_sem.at[g], volume.get((g, 1), 0), volume.get((g, 0), 0),
                        volume.get((g, -1), 0), extra_left)

    def y_arrived(dy):
        assert len(pieces(0, dy)) == len(pieces(1, dy))
        group_arrived(y_group[dy], len(pieces(0, dy)) * comps * reach)

    def feed_arrived():
        for z in range(nz):
            pl.when(at_left & (gz == z))(
                lambda z=z: settle(recv_sem.at[FEED], len(pieces(z, 0)) * comps * cells_y))

    lane = lax.broadcasted_iota(jnp.int32, (TILE, cells_z), 1)
    group = lane // GROUP
    mine = lax.rem(lane, GROUP) // half == gz
    held = ((lane >= jnp.where(gx == 0, cells_z - GROUP, cells_z))
            | (lane < jnp.where(gx == nx - 1, GROUP, 0)))
    is_first = lane >= jnp.where(gx == 0, 0, cells_z)
    is_last = lane >= jnp.where(gx == nx - 1, 0, cells_z)
    edge = lax.rem(lane + gz * (cells_z - DEPTH), cells_z) >= cells_z - DEPTH
    up_z = jnp.where(lane == 0, 0.0, COURANT)
    down_z = jnp.where(lane == cells_z - 1, 0.0, -COURANT)

    with scope("load_el"):
        load_e.wait()
        load_l.wait()
    weight = blend_ref[0]
    mixed = (1.0 - weight) * early[...] + weight * late[...]
    feed_send[...] = jnp.concatenate([mixed] * share, axis=2)

    with scope("load_v"):
        load_v.wait()
    swap = half + gz * (cells_z - GROUP)

    def turn(j):
        return (GROUP * j + half) % cells_z

    def pack(ring, c, rows):
        acc = None
        for j in range(groups):
            x = groups * ring + j
            p = first + x if x < cells_x + DEPTH else x - cells_x - DEPTH
            turned = pltpu.roll(cur[0, c, p, rows, :], turn(j), 1)
            acc = turned if acc is None else jnp.where(group == j, turned, acc)
        return acc

    def pack_rows(blocks):
        for r in blocks:
            outer = [[], []]
            for c in range(comps):
                packed = [pack(ring, c, pl.ds(r, TILE)) for ring in range(rings - 1)]
                for ring in range(rings - 1):
                    cur[0, c, strips + ring, pl.ds(r, TILE), :] = packed[ring]
                strip_send[c, pl.ds(r - TOP, TILE), :] = jnp.where(
                    mine, packed[0], pltpu.roll(packed[1], cells_z - half, 1))
                outer[0].append(packed[-1])
                outer[1].append(packed[0])
            for d in range(2):
                side = group >= groups // 2 if d == 0 else group < groups // 2
                strip_send[comps + d, pl.ds(r - TOP, TILE), :] = jnp.where(
                    side, jnp.where(mine, outer[d][0], pltpu.roll(outer[d][1], swap, 1)),
                    pltpu.roll(outer[d][2], cells_z // 2, 1))

    with scope("pack"):
        pack_rows([row_blocks[0], row_blocks[-1]])
    with scope("barrier"):
        await_greetings(barrier, expected)
    with scope("send"):
        start(y_strips[1], 0)
        start_feed(1, always, range(2, nx))
        start_feed(1, top, range(2))
        start(y_main[1], 0)
        start(y_strips[-1], 0)
        start_feed(-1, ~bottom)
        start(y_main[-1], 0)
        start_feed(0, always)
        start(x_messages, 0)
        for which, condition, where in late_greetings:
            greet(late_sem.at[which], condition, where)
    with scope("pack2"):
        pack_rows(row_blocks[1:-1])
    with scope("send2"):
        start(z_messages, 0)

    @pl.when((gx == 0) & needed(0))
    def _():
        feed_recv[0, :, own, :] = feed_send[...]

    def advance(q, behind, ahead, inner):
        scaled = [COURANT * q[d] for d in range(3)]
        weights = [jnp.abs(s) for s in scaled]
        keep = 1.0 - weights[0] - weights[1] - weights[2]
        if inner:
            weights[2] = jnp.maximum(up_z * q[2], down_z * q[2])
        positive = [q[d] > 0.0 for d in range(3)]
        result = []
        for c in range(comps):
            total = keep * q[c]
            for d in range(3):
                total += weights[d] * jnp.where(positive[d], behind[d][c], ahead[d][c])
            result.append(total)
        return result

    def shifted(t, p, r, dr, q):
        rows = r + dr
        if t == 0 and r in row_blocks and (rows < TOP or rows + TILE > TOP + cells_y):
            return [pltpu.roll(v, 1 if dr < 0 else TILE - 1, 0) for v in q]
        return [cur[t, c, p, pl.ds(rows, TILE), :] for c in range(comps)]

    def main(t, p, r):
        q, left, right = ([cur[t, c, p + dp, pl.ds(r, TILE), :] for c in range(comps)]
                          for dp in (0, -1, 1))
        behind = [left, shifted(t, p, r, -1, q), [pltpu.roll(v, 1, 1) for v in q]]
        ahead = [right, shifted(t, p, r, 1, q), [pltpu.roll(v, cells_z - 1, 1) for v in q]]
        return advance(q, behind, ahead, True)

    def merged(x, r, values):
        back = lax.rem(2 * cells_z - GROUP * lax.rem(x, groups) - half, cells_z)
        ring = strips + x // groups
        return [jnp.where(edge, pltpu.roll(cur[STEPS, c, ring, pl.ds(r, TILE), :], back, 1),
                          values[c]) for c in range(comps)]

    def plane(t, x, rows):
        for r in rows:
            values = main(t, x + first, r)
            if t < STEPS - 1:
                if isinstance(x, int) and x == -1:
                    values = [jnp.where(is_first, inflow[c, pl.ds(r, TILE), :], values[c])
                              for c in range(comps)]
                if isinstance(x, int) and x == cells_x:
                    values = [jnp.where(is_last, 0.0, v) for v in values]
                for c in range(comps):
                    cur[t + 1, c, x + first, pl.ds(r, TILE), :] = values[c]
                continue
            values = merged(x, r, values)
            for c in range(comps):
                if r == low_rows:
                    out_ref[c, x, 0:DEPTH, :] = values[c][TILE - DEPTH:]
                elif r == high_rows:
                    out_ref[c, x, cells_y - DEPTH:cells_y, :] = values[c][:DEPTH]
                else:
                    out_ref[c, x, pl.ds(r - TOP, TILE), :] = values[c]

    def planes(t, low, high, rows, unroll=None):
        cuts = sorted({low, high} | {k for k in (-1, 0, cells_x, cells_x + 1)
                                     if low < k < high})
        for begin, end in zip(cuts[:-1], cuts[1:]):
            if end - begin == 1:
                plane(t, begin, rows)
                continue

            def step(x, carry):
                plane(t, x, rows)
                return carry

            lax.fori_loop(begin, end, step, 0, unroll=unroll or end - begin)

    def around(t, r):
        ring = [[cur[t, c, strips + k, pl.ds(r, TILE), :] for c in range(comps)]
                for k in range(rings)]
        last = t == STEPS - 1

        def load(k, dr):
            return [cur[t, c, strips + k, pl.ds(r + dr, TILE), :] for c in range(comps)]

        for k in range(rings - 1 if last else rings):
            q, before, later = ring[k], ring[k - 1], ring[(k + 1) % rings]
            behind = [
                [pltpu.roll(jnp.where(group == groups - 1, before[c], q[c]), GROUP, 1)
                 for c in range(comps)],
                load(k, -1), [pltpu.roll(v, 1, 1) for v in q]]
            ahead = [
                [pltpu.roll(jnp.where(group == 0, later[c], q[c]), cells_z - GROUP, 1)
                 for c in range(comps)],
                load(k, 1), [pltpu.roll(v, cells_z - 1, 1) for v in q]]
            values = advance(q, behind, ahead, False)
            for c in range(comps):
                value = values[c]
                if k == rings - 1:
                    value = jnp.where(held, fixed[c, pl.ds(r, TILE), :], value)
                cur[t + 1, c, strips + k, pl.ds(r, TILE), :] = value

    def assemble(r):
        rows = pl.ds(r, TILE)
        low = group < groups // 2
        before, later = strip_recv[comps, rows, :], strip_recv[comps + 1, rows, :]
        mixed_far = jnp.where(low, later, before)
        far = [mixed_far, pltpu.roll(mixed_far, swap, 1),
               pltpu.roll(jnp.where(low, before, later), cells_z // 2, 1)]
        for c in range(comps):
            near = strip_recv[c, rows, :]
            theirs = [near, pltpu.roll(near, half, 1), far[c]]
            for ring in range(rings):
                if ring < rings - 1 and r in row_blocks:
                    ours = cur[0, c, strips + ring, rows, :]
                else:
                    ours = pack(ring, c, rows)
                value = jnp.where(mine, ours, theirs[ring])
                if ring == rings - 1:
                    value = jnp.where(held, fixed[c, rows, :], value)
                cur[0, c, strips + ring, rows, :] = value

    def ghosts(r):
        rows = pl.ds(r, TILE)
        for c in range(comps):
            values = feed_recv[gz * share, c, rows, :]
            for k in range(1, share):
                values = jnp.where(lane // piece == k,
                                   feed_recv[gz * share + k, c, rows, :], values)
            inflow[c, rows, :] = values
            beyond = feed_recv[share - gz, c, rows, :]
            there = turn(groups - 1)
            there_values = jnp.where(mine, pltpu.roll(values, there, 1),
                                     pltpu.roll(beyond, there, 1))
            fixed[c, rows, :] = jnp.where(is_first & (group == groups - 1), there_values, 0.0)
            cur[0, c, first - 1, rows, :] = jnp.where(
                is_first, values, cur[0, c, first - 1, rows, :])
            cur[0, c, after, rows, :] = jnp.where(is_last, 0.0, cur[0, c, after, rows, :])

    for t in range(STEPS - 1):
        with scope("A1_%d" % t):
            planes(t, t + 1, cells_x - 1 - t, row_blocks)

    with scope("late"):
        await_greetings(late_sem.at[NEAR], late_expected[NEAR])
        start(y_strips[1], 1)
        start_feed(1, ~top, range(2))
        for messages in (y_main[1], y_strips[-1], y_main[-1], z_messages, x_messages):
            start(messages, 1)

    @pl.when(bottom)
    def _():
        with scope("far"):
            await_greetings(late_sem.at[FAR], late_expected[FAR])
            start(y_strips[-1], 2)
            start_feed(-1, always)
            start(y_main[-1], 2)

    with scope("x_wait"):
        group_arrived(X)
    with scope("feed_wait"):
        feed_arrived()
    with scope("A2"):
        for r in row_blocks:
            ghosts(r)
        for t in range(STEPS - 1):
            beyond = STEPS - 1 - t
            planes(t, -beyond, t + 1, row_blocks)
            planes(t, cells_x - 1 - t, cells_x + beyond, row_blocks)
    with scope("z_wait"):
        group_arrived(Z)
    with scope("around"):
        for r in row_blocks:
            assemble(r)
        for t in range(STEPS):
            for r in row_blocks:
                around(t, r)
    with scope("final"):
        planes(STEPS - 1, 0, cells_x, row_blocks)

    def finish(dy):
        r = low_rows if dy > 0 else high_rows
        with scope("y_wait%d" % dy):
            y_arrived(dy)
        with scope("win%d" % dy):
            ghosts(r)
            assemble(r)
            for t in range(STEPS):
                beyond = STEPS - 1 - t
                around(t, r)
                planes(t, -beyond, cells_x + beyond, [r])

    @pl.when(bottom)
    def _():
        finish(-1)
        finish(1)

    @pl.when(~bottom)
    def _():
        finish(1)
        finish(-1)

    with scope("drain"):
        total = {dx: sum(rows for (_, d), rows in volume.items() if d == dx)
                 for dx in (-1, 0, 1)}
        settle_by_place(send_sem.at[0], total[-1], total[0], total[1])
        fed = comps * (cells_y + 2 * reach)
        pl.when(feeds)(lambda: settle(send_sem.at[1], fed))
        pl.when(at_left & needed(0))(lambda: settle(send_sem.at[1], 2 * comps * reach))


def local(sizes, velocity, plane_early, plane_late, blend):
    comps, cells_x, cells_y, cells_z = velocity.shape
    nx, ny, nz = sizes
    groups = cells_z // GROUP
    assert nz == 2 and ny > 2 and nx % nz == 0 and cells_z == 128
    assert cells_x == 2 * groups and 2 * DEPTH == groups and cells_y % TILE == 0
    dma = pltpu.SemaphoreType.DMA
    padded = cells_y + 2 * TOP
    planes = cells_x + 2 * DEPTH
    return pl.pallas_call(
        functools.partial(kernel, sizes),
        out_shape=pltpu.VMEM(velocity.shape, velocity.dtype),
        in_specs=[pl.BlockSpec(memory_space=pl.ANY)] * 3
        + [pl.BlockSpec(memory_space=pltpu.SMEM)],
        out_specs=pl.BlockSpec(memory_space=pltpu.VMEM),
        scratch_shapes=[
            pltpu.VMEM((STEPS + 1, comps, planes + 3, padded, cells_z), jnp.float32),
            pltpu.VMEM((comps + 2, cells_y, cells_z), jnp.float32),
            pltpu.VMEM((comps + 2, padded, cells_z), jnp.float32),
            pltpu.VMEM((comps, cells_y, cells_z), jnp.float32),
            pltpu.VMEM((nx, comps, padded, cells_z), jnp.float32),
            pltpu.VMEM((comps, padded, cells_z), jnp.float32),
            pltpu.VMEM((comps, padded, cells_z), jnp.float32),
            pltpu.VMEM(plane_early.shape, jnp.float32),
            pltpu.VMEM(plane_late.shape, jnp.float32),
            pltpu.VMEM((2 * comps * planes * padded, cells_z), jnp.float32),
            pltpu.SemaphoreType.REGULAR((2,)), dma((3,)), dma((2,)), dma((5,)),
        ],
        compiler_params=pltpu.CompilerParams(collective_id=0, has_side_effects=True),
        name="advect_substeps",
    )(velocity, plane_early, plane_late, blend)


def solution(mesh):
    sizes = tuple(mesh.shape[name] for name in ("gx", "gy", "gz"))
    return jax.shard_map(
        functools.partial(local, sizes),
        mesh=mesh,
        in_specs=(P(None, "gx", "gy", "gz"), P(None, "gy", "gx"), P(None, "gy", "gx"), P()),
        out_specs=P(None, "gx", "gy", "gz"),
        check_vma=False,
    )
```

```python
import functools

import jax
import jax.numpy as jnp
from jax import lax
from jax.experimental import pallas as pl
from jax.experimental.pallas import tpu as pltpu
from jax.sharding import PartitionSpec as P

STEPS = 4
COURANT = 0.08
DEPTH = STEPS
TILE = 8
TOP = 8
GROUP = 4 * DEPTH

MESH = pl.DeviceIdType.MESH
scope = jax.named_scope


def kernel(sizes, vel_hbm, early_hbm, late_hbm, blend_ref, out_ref,
           cur, strip_send, strip_recv, feed_send, feed_recv, inflow, fixed,
           early, late, tally, late_sem, load_sem, send_sem, recv_sem):
    nx, ny, nz = sizes
    comps, cells_x, cells_y, cells_z = vel_hbm.shape
    share = nx // nz
    piece = early_hbm.shape[2]
    feed_planes = -(-comps // share)
    gx, gy, gz = (lax.axis_index(name) for name in ("gx", "gy", "gz"))
    own = pl.ds(TOP, cells_y)
    first = DEPTH
    after = DEPTH + cells_x
    strips = cells_x + 2 * DEPTH
    groups = cells_z // GROUP
    rings = (cells_x + 2 * DEPTH) // groups
    half = GROUP // 2
    row_blocks = [TOP + TILE * b for b in range(cells_y // TILE)]
    low_rows, high_rows = TOP - DEPTH, TOP + cells_y - DEPTH

    load_v = pltpu.make_async_copy(
        vel_hbm, cur.at[0, :, pl.ds(first, cells_x), own, :], load_sem.at[0])
    load_e = pltpu.make_async_copy(early_hbm, early, load_sem.at[1])
    load_l = pltpu.make_async_copy(late_hbm, late, load_sem.at[2])
    load_v.start()
    load_e.start()
    load_l.start()

    has_left, has_right = gx > 0, gx < nx - 1
    always = gx >= 0
    others = {-1: has_left, 0: always, 1: has_right}
    bottom, top = gy == 0, gy == ny - 1

    def spanwise(dy):
        return lax.rem(gy + dy + ny, ny)

    def target(dx, dy, dz):
        where = {}
        if dx:
            where["gx"] = gx + dx
        if dy:
            where["gy"] = spanwise(dy)
        if dz:
            where["gz"] = 1 - gz
        return where

    def needed(k):
        return (k // share == gz) | (share - gz == k)

    feeds = (gx != 0) & needed(gx)

    def gain(dx, dy, dz):
        step = 2 * (lax.div(gx + dx + 2, 2) - lax.div(gx + 2, 2))
        if dy:
            step = step + spanwise(dy) - gy
        return step + 2 - 4 * gz if dz else step

    barrier = pltpu.get_barrier_semaphore()
    HOP, WIDE, FAR = 0, 1, 2
    expected = jnp.int32(0)
    late_expected = [jnp.int32(0)] * 3
    late_greetings = []
    soon, far = {}, {}

    def greet(semaphore, condition, where):
        @pl.when(condition)
        def _():
            pl.semaphore_signal(semaphore, 1, device_id=where, device_id_type=MESH)

    def await_greetings(semaphore, number):
        @pl.when(number > 0)
        def _():
            pl.semaphore_wait(semaphore, number)

    for dy in (-1, 1, 0):
        for dx in (0, -1, 1):
            for dz in (0, 1):
                place = (dx, dy, dz)
                if place == (0, 0, 0):
                    continue
                there, where, later = others[dx], target(*place), gain(*place)
                kind = HOP if abs(dx) + abs(dy) + dz == 1 else WIDE
                greet(barrier, there & (later >= 0), where)
                beyond = top if dy == 1 else gy < 0
                late_greetings.append((kind, there & (later < 0) & ~beyond, where))
                if dy == 1:
                    late_greetings.append((FAR, there & (later < 0) & beyond, where))
                soon[place] = later <= 0
                far[place] = (later > 0) & bottom if dy == -1 else gy < 0
                expected = expected + jnp.where(there & soon[place], 1, 0)
                late_expected[kind] = late_expected[kind] + jnp.where(
                    there & ~soon[place] & ~far[place], 1, 0)
                late_expected[FAR] = late_expected[FAR] + jnp.where(there & far[place], 1, 0)
    for k in range(2, nx):
        takes = (gx == 0) & needed(k)
        for dy in (-1, 1, 0):
            where = {"gx": k, "gy": spanwise(dy)}
            if dy == 1:
                greet(barrier, takes & ~top, where)
                late_greetings.append((FAR, takes & top, where))
            else:
                greet(barrier, takes, where)
        greet(barrier, (gx == k) & needed(k) & bottom, {"gx": 0, "gy": spanwise(-1)})
        expected = expected + jnp.where(takes & top, 1, 0)
    gives = (gx >= 2) & feeds
    expected = expected + jnp.where(gives, jnp.where(bottom, 2, 3), 0)
    late_expected[FAR] = late_expected[FAR] + jnp.where(gives & bottom, 1, 0)

    Y_UP, Y_DOWN, X_LEFT, X_RIGHT, Z, FEED = range(6)
    y_group = {1: Y_UP, -1: Y_DOWN}
    volume = {}

    def rows_of(ref):
        rows = 1
        for extent in ref.shape[:-1]:
            rows *= extent
        return rows

    def message(group, dx, dy, dz, src, dst):
        volume[group, dx] = volume.get((group, dx), 0) + rows_of(src)
        return (dx, dy, dz), pltpu.make_async_remote_copy(
            src_ref=src, dst_ref=dst, send_sem=send_sem.at[0], recv_sem=recv_sem.at[group],
            device_id=target(dx, dy, dz), device_id_type=MESH)

    def settle(semaphore, rows):
        part = tally.at[pl.ds(0, rows)]
        pltpu.make_async_copy(part, part, semaphore).wait()

    at_left, at_right = gx == 0, gx == nx - 1

    def settle_by_place(semaphore, from_left, middle, from_right, extra_left=0):
        pl.when(at_left)(lambda: settle(semaphore, middle + from_right + extra_left))
        pl.when(at_right)(lambda: settle(semaphore, middle + from_left))
        pl.when(~at_left & ~at_right)(
            lambda: settle(semaphore, middle + from_left + from_right))

    def rows_out(dy, depth, base):
        return pl.ds(base + cells_y - depth if dy > 0 else base, depth)

    def rows_in(dy, depth):
        return pl.ds(TOP - depth if dy > 0 else TOP + cells_y, depth)

    inside = pl.ds(first, cells_x)
    reach = DEPTH - 1
    y_main, y_strips = {}, {}
    for dy in (1, -1):
        g = y_group[dy]
        y_main[dy] = []
        for dx in (1, -1):
            for d in range(1, DEPTH):
                src = after - d if dx > 0 else first + d - 1
                dst = first - d if dx > 0 else after + d - 1
                y_main[dy].append(
                    message(g, dx, dy, 0, cur.at[0, :, src, rows_out(dy, DEPTH - d, TOP), :],
                            cur.at[0, :, dst, rows_in(dy, DEPTH - d), :]))
        y_main[dy].append(
            message(g, 0, dy, 0, cur.at[0, :, inside, rows_out(dy, DEPTH, TOP), :],
                    cur.at[0, :, inside, rows_in(dy, DEPTH), :]))
        y_strips[dy] = [
            message(g, 0, dy, 1, strip_send.at[pl.ds(0, comps), rows_out(dy, reach, 0), :],
                    strip_recv.at[pl.ds(0, comps), rows_in(dy, reach), :])]
        for dx in (1, -1):
            slot = comps if dx > 0 else comps + 1
            y_strips[dy].append(
                message(g, dx, dy, 1, strip_send.at[slot, rows_out(dy, reach - 1, 0), :],
                        strip_recv.at[slot, rows_in(dy, reach - 1), :]))
    x_messages = [
        message(X_LEFT, 1, 0, 0, cur.at[0, :, pl.ds(after - DEPTH, DEPTH), own, :],
                cur.at[0, :, pl.ds(0, DEPTH), own, :]),
        message(X_RIGHT, -1, 0, 0, cur.at[0, :, pl.ds(first, DEPTH), own, :],
                cur.at[0, :, pl.ds(after, DEPTH), own, :])]
    z_messages = [message(Z, 0, 0, 1, strip_send.at[pl.ds(0, comps)],
                          strip_recv.at[pl.ds(0, comps), own, :])]
    for dx in (1, -1):
        slot = comps if dx > 0 else comps + 1
        z_messages.append(
            message(Z, dx, 0, 1, strip_send.at[slot], strip_recv.at[slot, own, :]))

    def feed(k, dy, whole):
        where = {"gx": 0}
        if dy:
            where["gy"] = spanwise(dy)
        src = rows_out(dy, reach, 0) if dy else pl.ds(0, cells_y)
        dst = rows_in(dy, reach) if dy else own
        part = pl.ds(0, feed_planes) if whole else feed_planes
        return pltpu.make_async_remote_copy(
            src_ref=feed_send.at[part, src, :], dst_ref=feed_recv.at[k, part, dst, :],
            send_sem=send_sem.at[1], recv_sem=recv_sem.at[y_group[dy] if dy else FEED],
            device_id=where, device_id_type=MESH)

    def start_feed(dy, condition, ks=None, kinds=(False, True)):
        for k in ks or range(nx):
            for whole in kinds if k or dy else ():
                takes = k // share == gz if whole else share - gz == k
                pl.when((gx == k) & takes & condition)(feed(k, dy, whole).start)

    def fed_planes(z, local):
        total = 0
        for k in range(nx):
            if local or k:
                total += (feed_planes if k // share == z else 0) + (1 if share - z == k else 0)
        return total

    SOON = -1

    def start(messages, phase):
        for place, copy in messages:
            kind = HOP if sum(abs(d) for d in place) == 1 else WIDE
            if phase == SOON:
                when = soon[place]
            elif phase == FAR:
                when = far[place]
            elif phase == kind:
                when = ~soon[place] & ~far[place]
            else:
                continue
            pl.when(others[place[0]] & when)(copy.start)

    def group_arrived(g, extra_left=0):
        settle_by_place(recv_sem.at[g], volume.get((g, 1), 0), volume.get((g, 0), 0),
                        volume.get((g, -1), 0), extra_left)

    def y_arrived(dy):
        assert fed_planes(0, True) == fed_planes(1, True)
        group_arrived(y_group[dy], fed_planes(0, True) * reach)

    def feed_arrived():
        for z in range(nz):
            pl.when(at_left & (gz == z))(
                lambda z=z: settle(recv_sem.at[FEED], fed_planes(z, False) * cells_y))

    lane = lax.broadcasted_iota(jnp.int32, (TILE, cells_z), 1)
    group = lane // GROUP
    mine = lax.rem(lane, GROUP) // half == gz
    held = ((lane >= jnp.where(gx == 0, cells_z - GROUP, cells_z))
            | (lane < jnp.where(gx == nx - 1, GROUP, 0)))
    is_first = lane >= jnp.where(gx == 0, 0, cells_z)
    is_last = lane >= jnp.where(gx == nx - 1, 0, cells_z)
    edge = lax.rem(lane + gz * (cells_z - DEPTH), cells_z) >= cells_z - DEPTH
    up_z = jnp.where(lane == 0, 0.0, COURANT)
    down_z = jnp.where(lane == cells_z - 1, 0.0, -COURANT)

    def blend_piece():
        load_e.wait()
        load_l.wait()
        weight = blend_ref[0]
        mixed = (1.0 - weight) * early[...] + weight * late[...]
        for p in range(feed_planes):
            feed_send[p] = jnp.concatenate(
                [mixed[min(p * share + j, comps - 1)] for j in range(share)], axis=1)
        for b in range(cells_y // TILE):
            rows = slice(TILE * b, TILE * (b + 1))
            packed = jnp.zeros((TILE, cells_z), jnp.float32)
            for c in range(comps):
                repeated = jnp.concatenate([mixed[c, rows]] * share, axis=1)
                packed = jnp.where(
                    group == c, pltpu.roll(repeated, GROUP * c + half, 1), packed)
            feed_send[feed_planes, rows, :] = packed

    with scope("load_v"):
        load_v.wait()
    swap = half + gz * (cells_z - GROUP)

    def turn(j):
        return (GROUP * j + half) % cells_z

    def pack(ring, c, rows):
        acc = None
        for j in range(groups):
            x = groups * ring + j
            p = first + x if x < cells_x + DEPTH else x - cells_x - DEPTH
            turned = pltpu.roll(cur[0, c, p, rows, :], turn(j), 1)
            acc = turned if acc is None else jnp.where(group == j, turned, acc)
        return acc

    def pack_rows(blocks):
        for r in blocks:
            outer = [[], []]
            for c in range(comps):
                packed = [pack(ring, c, pl.ds(r, TILE)) for ring in range(rings - 1)]
                for ring in range(rings - 1):
                    cur[0, c, strips + ring, pl.ds(r, TILE), :] = packed[ring]
                strip_send[c, pl.ds(r - TOP, TILE), :] = jnp.where(
                    mine, packed[0], pltpu.roll(packed[1], cells_z - half, 1))
                outer[0].append(packed[-1])
                outer[1].append(packed[0])
            for d in range(2):
                side = group >= groups // 2 if d == 0 else group < groups // 2
                strip_send[comps + d, pl.ds(r - TOP, TILE), :] = jnp.where(
                    side, jnp.where(mine, outer[d][0], pltpu.roll(outer[d][1], swap, 1)),
                    pltpu.roll(outer[d][2], cells_z // 2, 1))

    with scope("pack"):
        pack_rows([row_blocks[0], row_blocks[-1]])
    with scope("blend"):
        blend_piece()

    @pl.when(bottom)
    def _():
        with scope("pack2"):
            pack_rows(row_blocks[1:-1])

    with scope("barrier"):
        await_greetings(barrier, expected)

    def start_up():
        start(y_strips[1], SOON)
        start_feed(1, always, range(2, nx))
        start_feed(1, top, range(2))
        start(y_main[1], SOON)

    def start_down():
        start(y_strips[-1], SOON)
        start_feed(-1, ~bottom)
        start(y_main[-1], SOON)

    with scope("send"):
        @pl.when(top)
        def _():
            start_up()
            start_down()

        @pl.when(~top)
        def _():
            start_down()
            start_up()

        start_feed(0, always, kinds=(False,))
        for which, condition, where in late_greetings:
            greet(late_sem.at[which], condition, where)

    @pl.when(~bottom)
    def _():
        with scope("pack2"):
            pack_rows(row_blocks[1:-1])

    with scope("send3"):
        start(z_messages[1:], SOON)
        start(x_messages, SOON)
        start_feed(0, always, kinds=(True,))
        start(z_messages[:1], SOON)

    @pl.when((gx == 0) & needed(0))
    def _():
        feed_recv[0, :, own, :] = feed_send[...]

    def advance(q, behind, ahead, inner):
        scaled = [COURANT * q[d] for d in range(3)]
        weights = [jnp.abs(s) for s in scaled]
        keep = 1.0 - weights[0] - weights[1] - weights[2]
        if inner:
            weights[2] = jnp.maximum(up_z * q[2], down_z * q[2])
        positive = [q[d] > 0.0 for d in range(3)]
        result = []
        for c in range(comps):
            total = keep * q[c]
            for d in range(3):
                total += weights[d] * jnp.where(positive[d], behind[d][c], ahead[d][c])
            result.append(total)
        return result

    def shifted(t, p, r, dr, q):
        rows = r + dr
        if t == 0 and r in row_blocks and (rows < TOP or rows + TILE > TOP + cells_y):
            return [pltpu.roll(v, 1 if dr < 0 else TILE - 1, 0) for v in q]
        return [cur[t, c, p, pl.ds(rows, TILE), :] for c in range(comps)]

    def main(t, p, r):
        q, left, right = ([cur[t, c, p + dp, pl.ds(r, TILE), :] for c in range(comps)]
                          for dp in (0, -1, 1))
        behind = [left, shifted(t, p, r, -1, q), [pltpu.roll(v, 1, 1) for v in q]]
        ahead = [right, shifted(t, p, r, 1, q), [pltpu.roll(v, cells_z - 1, 1) for v in q]]
        return advance(q, behind, ahead, True)

    def merged(x, r, values):
        back = (2 * cells_z - GROUP * (x % groups) - half) % cells_z
        ring = strips + x // groups
        return [jnp.where(edge, pltpu.roll(cur[STEPS, c, ring, pl.ds(r, TILE), :], back, 1),
                          values[c]) for c in range(comps)]

    def plane(t, x, rows):
        for r in rows:
            values = main(t, x + first, r)
            if t < STEPS - 1:
                if isinstance(x, int) and x == -1:
                    values = [jnp.where(is_first, inflow[c, pl.ds(r, TILE), :], values[c])
                              for c in range(comps)]
                if isinstance(x, int) and x == cells_x:
                    values = [jnp.where(is_last, 0.0, v) for v in values]
                for c in range(comps):
                    cur[t + 1, c, x + first, pl.ds(r, TILE), :] = values[c]
                continue
            if r in (low_rows, high_rows):
                values = merged(x, r, values)
            for c in range(comps):
                if r == low_rows:
                    out_ref[c, x, 0:DEPTH, :] = values[c][TILE - DEPTH:]
                elif r == high_rows:
                    out_ref[c, x, cells_y - DEPTH:cells_y, :] = values[c][:DEPTH]
                else:
                    out_ref[c, x, pl.ds(r - TOP, TILE), :] = values[c]

    def planes(t, low, high, rows, unroll=None):
        cuts = sorted({low, high} | {k for k in (-1, 0, cells_x, cells_x + 1)
                                     if low < k < high})
        for begin, end in zip(cuts[:-1], cuts[1:]):
            if end - begin == 1:
                plane(t, begin, rows)
                continue

            def step(x, carry):
                plane(t, x, rows)
                return carry

            lax.fori_loop(begin, end, step, 0, unroll=unroll or end - begin)

    def around(t, r):
        ring = [[cur[t, c, strips + k, pl.ds(r, TILE), :] for c in range(comps)]
                for k in range(rings)]
        last = t == STEPS - 1

        def load(k, dr):
            return [cur[t, c, strips + k, pl.ds(r + dr, TILE), :] for c in range(comps)]

        for k in range(rings - 1 if last else rings):
            q, before, later = ring[k], ring[k - 1], ring[(k + 1) % rings]
            behind = [
                [pltpu.roll(jnp.where(group == groups - 1, before[c], q[c]), GROUP, 1)
                 for c in range(comps)],
                load(k, -1), [pltpu.roll(v, 1, 1) for v in q]]
            ahead = [
                [pltpu.roll(jnp.where(group == 0, later[c], q[c]), cells_z - GROUP, 1)
                 for c in range(comps)],
                load(k, 1), [pltpu.roll(v, cells_z - 1, 1) for v in q]]
            values = advance(q, behind, ahead, False)
            for c in range(comps):
                value = values[c]
                if k == rings - 1:
                    value = jnp.where(held, fixed[c, pl.ds(r, TILE), :], value)
                cur[t + 1, c, strips + k, pl.ds(r, TILE), :] = value

    def assemble(r):
        rows = pl.ds(r, TILE)
        low = group < groups // 2
        before, later = strip_recv[comps, rows, :], strip_recv[comps + 1, rows, :]
        mixed_far = jnp.where(low, later, before)
        far = [mixed_far, pltpu.roll(mixed_far, swap, 1),
               pltpu.roll(jnp.where(low, before, later), cells_z // 2, 1)]
        for c in range(comps):
            near = strip_recv[c, rows, :]
            theirs = [near, pltpu.roll(near, half, 1), far[c]]
            for ring in range(rings):
                if ring < rings - 1 and r in row_blocks:
                    ours = cur[0, c, strips + ring, rows, :]
                else:
                    ours = pack(ring, c, rows)
                value = jnp.where(mine, ours, theirs[ring])
                if ring == rings - 1:
                    value = jnp.where(held, fixed[c, rows, :], value)
                cur[0, c, strips + ring, rows, :] = value

    def ghosts(r):
        rows = pl.ds(r, TILE)
        for c in range(comps):
            for k in range(share):
                part = feed_recv[gz * share + k, c // share, rows, :]
                if k != c % share:
                    part = pltpu.roll(part, (k - c % share) * piece % cells_z, 1)
                values = part if k == 0 else jnp.where(lane // piece == k, part, values)
            inflow[c, rows, :] = values
            beyond = feed_recv[share - gz, feed_planes, rows, :]
            there_values = jnp.where(mine, pltpu.roll(values, turn(groups - 1), 1),
                                     pltpu.roll(beyond, GROUP * (groups - 1 - c), 1))
            fixed[c, rows, :] = jnp.where(is_first & (group == groups - 1), there_values, 0.0)
            cur[0, c, first - 1, rows, :] = jnp.where(
                is_first, values, cur[0, c, first - 1, rows, :])

    def end_ghost(r):
        rows = pl.ds(r, TILE)
        for c in range(comps):
            cur[0, c, after, rows, :] = jnp.where(is_last, 0.0, cur[0, c, after, rows, :])

    final_blocks = range(TOP + DEPTH, TOP + cells_y - DEPTH, TILE)

    def blocks_of(t):
        return row_blocks if t < STEPS - 1 else final_blocks

    for t in range(STEPS):
        with scope("A1_%d" % t):
            planes(t, t + 1, cells_x - 1 - t, blocks_of(t))

    with scope("late_hop"):
        await_greetings(late_sem.at[HOP], late_expected[HOP])
        start_feed(1, ~top, [0])
        for messages in (y_main[1], y_main[-1], x_messages, z_messages):
            start(messages, HOP)
    with scope("late_wide"):
        await_greetings(late_sem.at[WIDE], late_expected[WIDE])
        start(y_strips[1], WIDE)
        start_feed(1, ~top, [1])
        for messages in (y_main[1], y_strips[-1], y_main[-1], z_messages):
            start(messages, WIDE)

    def across():
        @pl.when(bottom)
        def _():
            with scope("far"):
                await_greetings(late_sem.at[FAR], late_expected[FAR])
                start(y_strips[-1], FAR)
                start_feed(-1, always)
                start(y_main[-1], FAR)

    def left_side():
        with scope("left_wait"):
            pl.when(has_left)(lambda: settle(recv_sem.at[X_LEFT], volume[X_LEFT, 1]))
            feed_arrived()
        with scope("left"):
            for r in row_blocks:
                ghosts(r)
            for t in range(STEPS):
                planes(t, t + 1 - STEPS, t + 1, blocks_of(t))

    def right_side():
        with scope("right_wait"):
            pl.when(has_right)(lambda: settle(recv_sem.at[X_RIGHT], volume[X_RIGHT, -1]))
        with scope("right"):
            for r in row_blocks:
                end_ghost(r)
            for t in range(STEPS):
                planes(t, cells_x - 1 - t, cells_x - 1 - t + STEPS, blocks_of(t))

    @pl.when(lax.rem(gx, 2) == 0)
    def _():
        right_side()
        across()
        left_side()

    @pl.when(lax.rem(gx, 2) == 1)
    def _():
        left_side()
        across()
        right_side()

    with scope("z_wait"):
        group_arrived(Z)
    with scope("around"):
        for r in row_blocks:
            assemble(r)
        for t in range(STEPS):
            for r in blocks_of(t):
                around(t, r)
        for x in range(cells_x):
            for r in final_blocks:
                rows = pl.ds(r - TOP, TILE)
                values = merged(x, r, [out_ref[c, x, rows, :] for c in range(comps)])
                for c in range(comps):
                    out_ref[c, x, rows, :] = values[c]

    def finish(dy):
        r = low_rows if dy > 0 else high_rows
        with scope("y_wait%d" % dy):
            y_arrived(dy)
        with scope("win%d" % dy):
            ghosts(r)
            end_ghost(r)
            assemble(r)
            for t in range(STEPS):
                beyond = STEPS - 1 - t
                around(t, r)
                planes(t, -beyond, cells_x + beyond, [r])

    @pl.when(bottom)
    def _():
        finish(-1)
        finish(1)

    @pl.when(~bottom)
    def _():
        finish(1)
        finish(-1)

    with scope("drain"):
        total = {dx: sum(rows for (_, d), rows in volume.items() if d == dx)
                 for dx in (-1, 0, 1)}
        settle_by_place(send_sem.at[0], total[-1], total[0], total[1])
        fed = cells_y + 2 * reach
        whole = lax.div(gx, share) == gz
        pl.when(~at_left & whole)(lambda: settle(send_sem.at[1], feed_planes * fed))
        pl.when(~at_left & (share - gz == gx))(lambda: settle(send_sem.at[1], fed))
        pl.when(at_left & whole)(lambda: settle(send_sem.at[1], 2 * feed_planes * reach))
        if share == 1:
            pl.when(at_left & (gz == 1))(lambda: settle(send_sem.at[1], 2 * reach))


def local(sizes, velocity, plane_early, plane_late, blend):
    comps, cells_x, cells_y, cells_z = velocity.shape
    nx, ny, nz = sizes
    groups = cells_z // GROUP
    assert nz == 2 and ny > 2 and nx % nz == 0 and cells_z == 128
    assert cells_x == 2 * groups and 2 * DEPTH == groups and cells_y % TILE == 0
    assert TILE == 2 * DEPTH and comps <= groups
    share = nx // nz
    feed_planes = -(-comps // share)
    assert plane_early.shape[2] * share == cells_z
    dma = pltpu.SemaphoreType.DMA
    padded = cells_y + 2 * TOP
    planes = cells_x + 2 * DEPTH
    return pl.pallas_call(
        functools.partial(kernel, sizes),
        out_shape=pltpu.VMEM(velocity.shape, velocity.dtype),
        in_specs=[pl.BlockSpec(memory_space=pl.ANY)] * 3
        + [pl.BlockSpec(memory_space=pltpu.SMEM)],
        out_specs=pl.BlockSpec(memory_space=pltpu.VMEM),
        scratch_shapes=[
            pltpu.VMEM((STEPS + 1, comps, planes + 3, padded, cells_z), jnp.float32),
            pltpu.VMEM((comps + 2, cells_y, cells_z), jnp.float32),
            pltpu.VMEM((comps + 2, padded, cells_z), jnp.float32),
            pltpu.VMEM((feed_planes + 1, cells_y, cells_z), jnp.float32),
            pltpu.VMEM((nx, feed_planes + 1, padded, cells_z), jnp.float32),
            pltpu.VMEM((comps, padded, cells_z), jnp.float32),
            pltpu.VMEM((comps, padded, cells_z), jnp.float32),
            pltpu.VMEM(plane_early.shape, jnp.float32),
            pltpu.VMEM(plane_late.shape, jnp.float32),
            pltpu.VMEM((2 * comps * planes * padded, cells_z), jnp.float32),
            pltpu.SemaphoreType.REGULAR((3,)), dma((3,)), dma((2,)), dma((6,)),
        ],
        compiler_params=pltpu.CompilerParams(collective_id=0, has_side_effects=True),
        name="advect_substeps",
    )(velocity, plane_early, plane_late, blend)


def solution(mesh):
    sizes = tuple(mesh.shape[name] for name in ("gx", "gy", "gz"))
    return jax.shard_map(
        functools.partial(local, sizes),
        mesh=mesh,
        in_specs=(P(None, "gx", "gy", "gz"), P(None, "gy", "gx"), P(None, "gy", "gx"), P()),
        out_specs=P(None, "gx", "gy", "gz"),
        check_vma=False,
    )
```

```python
import functools

import jax
import jax.numpy as jnp
from jax import lax
from jax.experimental import pallas as pl
from jax.experimental.pallas import tpu as pltpu
from jax.sharding import PartitionSpec as P

STEPS = 4
COURANT = 0.08
DEPTH = STEPS
TILE = 8
TOP = 8
GROUP = 4 * DEPTH

MESH = pl.DeviceIdType.MESH
scope = jax.named_scope


def kernel(sizes, vel_hbm, early_hbm, late_hbm, blend_ref, out_ref,
           cur, strip_send, strip_recv, feed_send, feed_recv, inflow, fixed,
           early, late, tally, late_sem, load_sem, send_sem, recv_sem):
    nx, ny, nz = sizes
    comps, cells_x, cells_y, cells_z = vel_hbm.shape
    share = nx // nz
    piece = early_hbm.shape[2]
    feed_planes = -(-comps // share)
    gx, gy, gz = (lax.axis_index(name) for name in ("gx", "gy", "gz"))
    own = pl.ds(TOP, cells_y)
    first = DEPTH
    after = DEPTH + cells_x
    strips = cells_x + 2 * DEPTH
    groups = cells_z // GROUP
    rings = (cells_x + 2 * DEPTH) // groups
    half = GROUP // 2
    row_blocks = [TOP + TILE * b for b in range(cells_y // TILE)]
    low_rows, high_rows = TOP - DEPTH, TOP + cells_y - DEPTH

    load_v = pltpu.make_async_copy(
        vel_hbm, cur.at[0, :, pl.ds(first, cells_x), own, :], load_sem.at[0])
    load_e = pltpu.make_async_copy(early_hbm, early, load_sem.at[1])
    load_l = pltpu.make_async_copy(late_hbm, late, load_sem.at[2])
    load_e.start()
    load_l.start()
    load_v.start()

    has_left, has_right = gx > 0, gx < nx - 1
    always = gx >= 0
    others = {-1: has_left, 0: always, 1: has_right}
    bottom, top = gy == 0, gy == ny - 1

    def spanwise(dy):
        return lax.rem(gy + dy + ny, ny)

    def target(dx, dy, dz):
        where = {}
        if dx:
            where["gx"] = gx + dx
        if dy:
            where["gy"] = spanwise(dy)
        if dz:
            where["gz"] = 1 - gz
        return where

    def needed(k):
        return (k // share == gz) | (share - gz == k)

    feeds = (gx != 0) & needed(gx)

    def gain(dx, dy, dz):
        step = 2 * (lax.div(gx + dx + 2, 2) - lax.div(gx + 2, 2))
        if dy:
            rows = spanwise(dy) - gy
            step = step + jnp.where(top if dy > 0 else bottom, 8 * rows, rows)
        return step + 2 - 4 * gz if dz else step

    barrier = pltpu.get_barrier_semaphore()
    HOP, WIDE, FAR = 0, 1, 2
    expected = jnp.int32(0)
    late_expected = [jnp.int32(0)] * 3
    late_greetings = []
    soon, far = {}, {}

    def greet(semaphore, condition, where):
        @pl.when(condition)
        def _():
            pl.semaphore_signal(semaphore, 1, device_id=where, device_id_type=MESH)

    def await_greetings(semaphore, number):
        @pl.when(number > 0)
        def _():
            pl.semaphore_wait(semaphore, number)

    for dy in (-1, 1, 0):
        for dx in (0, -1, 1):
            for dz in (0, 1):
                place = (dx, dy, dz)
                if place == (0, 0, 0):
                    continue
                there, where, later = others[dx], target(*place), gain(*place)
                kind = HOP if abs(dx) + abs(dy) + dz == 1 else WIDE
                greet(barrier, there & (later >= 0), where)
                beyond = top if dy == 1 else gy < 0
                late_greetings.append((kind, there & (later < 0) & ~beyond, where))
                if dy == 1:
                    late_greetings.append((FAR, there & (later < 0) & beyond, where))
                soon[place] = later <= 0
                far[place] = (later > 0) & bottom if dy == -1 else gy < 0
                expected = expected + jnp.where(there & soon[place], 1, 0)
                late_expected[kind] = late_expected[kind] + jnp.where(
                    there & ~soon[place] & ~far[place], 1, 0)
                late_expected[FAR] = late_expected[FAR] + jnp.where(there & far[place], 1, 0)
    for k in range(2, nx):
        takes = (gx == 0) & needed(k)
        for dy in (-1, 1, 0):
            where = {"gx": k, "gy": spanwise(dy)}
            if dy == 1:
                greet(barrier, takes & ~top, where)
                late_greetings.append((FAR, takes & top, where))
            else:
                greet(barrier, takes, where)
        greet(barrier, (gx == k) & needed(k) & bottom, {"gx": 0, "gy": spanwise(-1)})
        expected = expected + jnp.where(takes & top, 1, 0)
    gives = (gx >= 2) & feeds
    expected = expected + jnp.where(gives, jnp.where(bottom, 2, 3), 0)
    late_expected[FAR] = late_expected[FAR] + jnp.where(gives & bottom, 1, 0)

    Y_UP, Y_DOWN, X_LEFT, X_RIGHT, Z, FEED = range(6)
    y_group = {1: Y_UP, -1: Y_DOWN}
    volume = {}

    def rows_of(ref):
        rows = 1
        for extent in ref.shape[:-1]:
            rows *= extent
        return rows

    def message(group, dx, dy, dz, src, dst):
        volume[group, dx] = volume.get((group, dx), 0) + rows_of(src)
        return (dx, dy, dz), pltpu.make_async_remote_copy(
            src_ref=src, dst_ref=dst, send_sem=send_sem.at[0], recv_sem=recv_sem.at[group],
            device_id=target(dx, dy, dz), device_id_type=MESH)

    def settle(semaphore, rows):
        part = tally.at[pl.ds(0, rows)]
        pltpu.make_async_copy(part, part, semaphore).wait()

    at_left, at_right = gx == 0, gx == nx - 1

    def settle_by_place(semaphore, from_left, middle, from_right, extra_left=0):
        pl.when(at_left)(lambda: settle(semaphore, middle + from_right + extra_left))
        pl.when(at_right)(lambda: settle(semaphore, middle + from_left))
        pl.when(~at_left & ~at_right)(
            lambda: settle(semaphore, middle + from_left + from_right))

    def rows_out(dy, depth, base):
        return pl.ds(base + cells_y - depth if dy > 0 else base, depth)

    def rows_in(dy, depth):
        return pl.ds(TOP - depth if dy > 0 else TOP + cells_y, depth)

    inside = pl.ds(first, cells_x)
    reach = DEPTH - 1
    y_main, y_strips = {}, {}
    for dy in (1, -1):
        g = y_group[dy]
        y_main[dy] = []
        for dx in (1, -1):
            for d in range(1, DEPTH):
                src = after - d if dx > 0 else first + d - 1
                dst = first - d if dx > 0 else after + d - 1
                y_main[dy].append(
                    message(g, dx, dy, 0, cur.at[0, :, src, rows_out(dy, DEPTH - d, TOP), :],
                            cur.at[0, :, dst, rows_in(dy, DEPTH - d), :]))
        y_main[dy].append(
            message(g, 0, dy, 0, cur.at[0, :, inside, rows_out(dy, DEPTH, TOP), :],
                    cur.at[0, :, inside, rows_in(dy, DEPTH), :]))
        y_strips[dy] = [
            message(g, 0, dy, 1, strip_send.at[pl.ds(0, comps), rows_out(dy, reach, 0), :],
                    strip_recv.at[pl.ds(0, comps), rows_in(dy, reach), :])]
        for dx in (1, -1):
            slot = comps if dx > 0 else comps + 1
            y_strips[dy].append(
                message(g, dx, dy, 1, strip_send.at[slot, rows_out(dy, reach - 1, 0), :],
                        strip_recv.at[slot, rows_in(dy, reach - 1), :]))
    x_messages = [
        message(X_LEFT, 1, 0, 0, cur.at[0, :, pl.ds(after - DEPTH, DEPTH), own, :],
                cur.at[0, :, pl.ds(0, DEPTH), own, :]),
        message(X_RIGHT, -1, 0, 0, cur.at[0, :, pl.ds(first, DEPTH), own, :],
                cur.at[0, :, pl.ds(after, DEPTH), own, :])]
    z_messages = [message(Z, 0, 0, 1, strip_send.at[pl.ds(0, comps)],
                          strip_recv.at[pl.ds(0, comps), own, :])]
    for dx in (1, -1):
        slot = comps if dx > 0 else comps + 1
        z_messages.append(
            message(Z, dx, 0, 1, strip_send.at[slot], strip_recv.at[slot, own, :]))

    def feed(k, dy, whole):
        where = {"gx": 0}
        if dy:
            where["gy"] = spanwise(dy)
        src = rows_out(dy, reach, 0) if dy else pl.ds(0, cells_y)
        dst = rows_in(dy, reach) if dy else own
        part = pl.ds(0, feed_planes) if whole else feed_planes
        return pltpu.make_async_remote_copy(
            src_ref=feed_send.at[part, src, :], dst_ref=feed_recv.at[k, part, dst, :],
            send_sem=send_sem.at[1], recv_sem=recv_sem.at[y_group[dy] if dy else FEED],
            device_id=where, device_id_type=MESH)

    def start_feed(dy, condition, ks=None, kinds=(False, True)):
        for k in ks or range(nx):
            for whole in kinds if k or dy else ():
                takes = k // share == gz if whole else share - gz == k
                pl.when((gx == k) & takes & condition)(feed(k, dy, whole).start)

    def fed_planes(z, local):
        total = 0
        for k in range(nx):
            if local or k:
                total += (feed_planes if k // share == z else 0) + (1 if share - z == k else 0)
        return total

    SOON = -1

    def start(messages, phase):
        for place, copy in messages:
            kind = HOP if sum(abs(d) for d in place) == 1 else WIDE
            if phase == SOON:
                when = soon[place]
            elif phase == FAR:
                when = far[place]
            elif phase == kind:
                when = ~soon[place] & ~far[place]
            else:
                continue
            pl.when(others[place[0]] & when)(copy.start)

    def group_arrived(g, extra_left=0):
        settle_by_place(recv_sem.at[g], volume.get((g, 1), 0), volume.get((g, 0), 0),
                        volume.get((g, -1), 0), extra_left)

    def y_arrived(dy):
        assert fed_planes(0, True) == fed_planes(1, True)
        group_arrived(y_group[dy], fed_planes(0, True) * reach)

    def feed_arrived():
        for z in range(nz):
            pl.when(at_left & (gz == z))(
                lambda z=z: settle(recv_sem.at[FEED], fed_planes(z, False) * cells_y))

    lane = lax.broadcasted_iota(jnp.int32, (TILE, cells_z), 1)
    group = lane // GROUP
    mine = lax.rem(lane, GROUP) // half == gz
    held = ((lane >= jnp.where(gx == 0, cells_z - GROUP, cells_z))
            | (lane < jnp.where(gx == nx - 1, GROUP, 0)))
    is_first = lane >= jnp.where(gx == 0, 0, cells_z)
    is_last = lane >= jnp.where(gx == nx - 1, 0, cells_z)
    edge = lax.rem(lane + gz * (cells_z - DEPTH), cells_z) >= cells_z - DEPTH
    up_z = jnp.where(lane == 0, 0.0, COURANT)
    down_z = jnp.where(lane == cells_z - 1, 0.0, -COURANT)

    def blend_piece():
        load_e.wait()
        load_l.wait()
        weight = blend_ref[0]
        mixed = (1.0 - weight) * early[...] + weight * late[...]
        for p in range(feed_planes):
            feed_send[p] = jnp.concatenate(
                [mixed[min(p * share + j, comps - 1)] for j in range(share)], axis=1)
        for b in range(cells_y // TILE):
            rows = slice(TILE * b, TILE * (b + 1))
            packed = jnp.zeros((TILE, cells_z), jnp.float32)
            for c in range(comps):
                repeated = jnp.concatenate([mixed[c, rows]] * share, axis=1)
                packed = jnp.where(
                    group == c, pltpu.roll(repeated, GROUP * c + half, 1), packed)
            feed_send[feed_planes, rows, :] = packed

    with scope("blend"):
        blend_piece()
    with scope("load_v"):
        load_v.wait()
    swap = half + gz * (cells_z - GROUP)

    def turn(j):
        return (GROUP * j + half) % cells_z

    def pack(ring, c, rows):
        acc = None
        for j in range(groups):
            x = groups * ring + j
            p = first + x if x < cells_x + DEPTH else x - cells_x - DEPTH
            turned = pltpu.roll(cur[0, c, p, rows, :], turn(j), 1)
            acc = turned if acc is None else jnp.where(group == j, turned, acc)
        return acc

    def pack_rows(blocks):
        for r in blocks:
            outer = [[], []]
            for c in range(comps):
                packed = [pack(ring, c, pl.ds(r, TILE)) for ring in range(rings - 1)]
                for ring in range(rings - 1):
                    cur[0, c, strips + ring, pl.ds(r, TILE), :] = packed[ring]
                strip_send[c, pl.ds(r - TOP, TILE), :] = jnp.where(
                    mine, packed[0], pltpu.roll(packed[1], cells_z - half, 1))
                outer[0].append(packed[-1])
                outer[1].append(packed[0])
            for d in range(2):
                side = group >= groups // 2 if d == 0 else group < groups // 2
                strip_send[comps + d, pl.ds(r - TOP, TILE), :] = jnp.where(
                    side, jnp.where(mine, outer[d][0], pltpu.roll(outer[d][1], swap, 1)),
                    pltpu.roll(outer[d][2], cells_z // 2, 1))

    def enter():
        with scope("barrier"):
            await_greetings(barrier, expected)

    def start_up():
        start(y_strips[1], SOON)
        start_feed(1, always, range(2, nx))
        start_feed(1, top, range(2))
        start(y_main[1], SOON)

    def start_down():
        start(y_strips[-1], SOON)
        start_feed(-1, ~bottom)
        start(y_main[-1], SOON)

    def greet_late():
        for which, condition, where in late_greetings:
            greet(late_sem.at[which], condition, where)

    def start_across():
        start(z_messages[1:], SOON)
        start(x_messages, SOON)
        start_feed(0, always, kinds=(True,))
        start(z_messages[:1], SOON)

    @pl.when(bottom)
    def _():
        with scope("pack"):
            pack_rows([row_blocks[0], row_blocks[-1]])
        with scope("pack2"):
            pack_rows(row_blocks[1:-1])
        enter()
        with scope("send"):
            start_feed(0, always, kinds=(False,))
            start_across()
            greet_late()
            start_up()
            start_down()

    @pl.when(~bottom)
    def _():
        @pl.when(top)
        def _():
            pack_rows(row_blocks[-1:])
            enter()
            start_up()
            pack_rows(row_blocks[:1])
            start_down()

        @pl.when(~top)
        def _():
            pack_rows(row_blocks[:1])
            enter()
            start_down()
            pack_rows(row_blocks[-1:])
            start_up()

        with scope("send"):
            start_feed(0, always, kinds=(False,))
            greet_late()
        with scope("pack2"):
            pack_rows(row_blocks[1:-1])
        with scope("send3"):
            start_across()

    @pl.when((gx == 0) & needed(0))
    def _():
        feed_recv[0, :, own, :] = feed_send[...]

    def advance(q, behind, ahead, inner):
        scaled = [COURANT * q[d] for d in range(3)]
        weights = [jnp.abs(s) for s in scaled]
        keep = 1.0 - weights[0] - weights[1] - weights[2]
        if inner:
            weights[2] = jnp.maximum(up_z * q[2], down_z * q[2])
        positive = [q[d] > 0.0 for d in range(3)]
        result = []
        for c in range(comps):
            total = keep * q[c]
            for d in range(3):
                total += weights[d] * jnp.where(positive[d], behind[d][c], ahead[d][c])
            result.append(total)
        return result

    def shifted(t, p, r, dr, q):
        rows = r + dr
        if t == 0 and r in row_blocks and (rows < TOP or rows + TILE > TOP + cells_y):
            return [pltpu.roll(v, 1 if dr < 0 else TILE - 1, 0) for v in q]
        return [cur[t, c, p, pl.ds(rows, TILE), :] for c in range(comps)]

    def main(t, p, r):
        q, left, right = ([cur[t, c, p + dp, pl.ds(r, TILE), :] for c in range(comps)]
                          for dp in (0, -1, 1))
        behind = [left, shifted(t, p, r, -1, q), [pltpu.roll(v, 1, 1) for v in q]]
        ahead = [right, shifted(t, p, r, 1, q), [pltpu.roll(v, cells_z - 1, 1) for v in q]]
        return advance(q, behind, ahead, True)

    def merged(x, r, values):
        back = (2 * cells_z - GROUP * (x % groups) - half) % cells_z
        ring = strips + x // groups
        return [jnp.where(edge, pltpu.roll(cur[STEPS, c, ring, pl.ds(r, TILE), :], back, 1),
                          values[c]) for c in range(comps)]

    def plane(t, x, rows):
        for r in rows:
            values = main(t, x + first, r)
            if t < STEPS - 1:
                if isinstance(x, int) and x == -1:
                    values = [jnp.where(is_first, inflow[c, pl.ds(r, TILE), :], values[c])
                              for c in range(comps)]
                if isinstance(x, int) and x == cells_x:
                    values = [jnp.where(is_last, 0.0, v) for v in values]
                for c in range(comps):
                    cur[t + 1, c, x + first, pl.ds(r, TILE), :] = values[c]
                continue
            if r in (low_rows, high_rows):
                values = merged(x, r, values)
            for c in range(comps):
                if r == low_rows:
                    out_ref[c, x, 0:DEPTH, :] = values[c][TILE - DEPTH:]
                elif r == high_rows:
                    out_ref[c, x, cells_y - DEPTH:cells_y, :] = values[c][:DEPTH]
                else:
                    out_ref[c, x, pl.ds(r - TOP, TILE), :] = values[c]

    def planes(t, low, high, rows, unroll=None):
        cuts = sorted({low, high} | {k for k in (-1, 0, cells_x, cells_x + 1)
                                     if low < k < high})
        for begin, end in zip(cuts[:-1], cuts[1:]):
            if end - begin == 1:
                plane(t, begin, rows)
                continue

            def step(x, carry):
                plane(t, x, rows)
                return carry

            lax.fori_loop(begin, end, step, 0, unroll=unroll or end - begin)

    def around(t, r):
        ring = [[cur[t, c, strips + k, pl.ds(r, TILE), :] for c in range(comps)]
                for k in range(rings)]
        last = t == STEPS - 1

        def load(k, dr):
            return [cur[t, c, strips + k, pl.ds(r + dr, TILE), :] for c in range(comps)]

        for k in range(rings - 1 if last else rings):
            q, before, later = ring[k], ring[k - 1], ring[(k + 1) % rings]
            behind = [
                [pltpu.roll(jnp.where(group == groups - 1, before[c], q[c]), GROUP, 1)
                 for c in range(comps)],
                load(k, -1), [pltpu.roll(v, 1, 1) for v in q]]
            ahead = [
                [pltpu.roll(jnp.where(group == 0, later[c], q[c]), cells_z - GROUP, 1)
                 for c in range(comps)],
                load(k, 1), [pltpu.roll(v, cells_z - 1, 1) for v in q]]
            values = advance(q, behind, ahead, False)
            for c in range(comps):
                value = values[c]
                if k == rings - 1:
                    value = jnp.where(held, fixed[c, pl.ds(r, TILE), :], value)
                cur[t + 1, c, strips + k, pl.ds(r, TILE), :] = value

    def assemble(r):
        rows = pl.ds(r, TILE)
        low = group < groups // 2
        before, later = strip_recv[comps, rows, :], strip_recv[comps + 1, rows, :]
        mixed_far = jnp.where(low, later, before)
        far = [mixed_far, pltpu.roll(mixed_far, swap, 1),
               pltpu.roll(jnp.where(low, before, later), cells_z // 2, 1)]
        for c in range(comps):
            near = strip_recv[c, rows, :]
            theirs = [near, pltpu.roll(near, half, 1), far[c]]
            for ring in range(rings):
                if ring < rings - 1 and r in row_blocks:
                    ours = cur[0, c, strips + ring, rows, :]
                else:
                    ours = pack(ring, c, rows)
                value = jnp.where(mine, ours, theirs[ring])
                if ring == rings - 1:
                    value = jnp.where(held, fixed[c, rows, :], value)
                cur[0, c, strips + ring, rows, :] = value

    def ghosts(r):
        rows = pl.ds(r, TILE)
        for c in range(comps):
            for k in range(share):
                part = feed_recv[gz * share + k, c // share, rows, :]
                if k != c % share:
                    part = pltpu.roll(part, (k - c % share) * piece % cells_z, 1)
                values = part if k == 0 else jnp.where(lane // piece == k, part, values)
            inflow[c, rows, :] = values
            beyond = feed_recv[share - gz, feed_planes, rows, :]
            there_values = jnp.where(mine, pltpu.roll(values, turn(groups - 1), 1),
                                     pltpu.roll(beyond, GROUP * (groups - 1 - c), 1))
            fixed[c, rows, :] = jnp.where(is_first & (group == groups - 1), there_values, 0.0)
            cur[0, c, first - 1, rows, :] = jnp.where(
                is_first, values, cur[0, c, first - 1, rows, :])

    def end_ghost(r):
        rows = pl.ds(r, TILE)
        for c in range(comps):
            cur[0, c, after, rows, :] = jnp.where(is_last, 0.0, cur[0, c, after, rows, :])

    final_blocks = range(TOP + DEPTH, TOP + cells_y - DEPTH, TILE)

    def blocks_of(t):
        return row_blocks if t < STEPS - 1 else final_blocks

    for t in range(STEPS):
        with scope("A1_%d" % t):
            planes(t, t + 1, cells_x - 1 - t, blocks_of(t))

    with scope("late_hop"):
        await_greetings(late_sem.at[HOP], late_expected[HOP])
        start_feed(1, ~top, [0])
        for messages in (y_main[1], y_main[-1], x_messages, z_messages):
            start(messages, HOP)
    with scope("late_wide"):
        await_greetings(late_sem.at[WIDE], late_expected[WIDE])
        start(y_strips[1], WIDE)
        start_feed(1, ~top, [1])
        for messages in (y_main[1], y_strips[-1], y_main[-1], z_messages):
            start(messages, WIDE)

    def across(z):
        @pl.when(bottom & (gz == z))
        def _():
            with scope("far"):
                await_greetings(late_sem.at[FAR], late_expected[FAR])
                start(y_strips[-1], FAR)
                start_feed(-1, always)
                start(y_main[-1], FAR)

    def left_side():
        with scope("left_wait"):
            pl.when(has_left)(lambda: settle(recv_sem.at[X_LEFT], volume[X_LEFT, 1]))
            feed_arrived()
        with scope("left"):
            pl.when(gx == 0)(lambda: across(1))
            for r in row_blocks:
                ghosts(r)
            for t in range(STEPS):
                planes(t, t + 1 - STEPS, t + 1, blocks_of(t))

    def right_side():
        with scope("right_wait"):
            pl.when(has_right)(lambda: settle(recv_sem.at[X_RIGHT], volume[X_RIGHT, -1]))
        with scope("right"):
            pl.when(gx == 1)(lambda: across(1))
            for r in row_blocks:
                end_ghost(r)
            for t in range(STEPS):
                planes(t, cells_x - 1 - t, cells_x - 1 - t + STEPS, blocks_of(t))

    @pl.when(lax.rem(gx, 2) == 0)
    def _():
        right_side()
        across(0)
        left_side()

    @pl.when(lax.rem(gx, 2) == 1)
    def _():
        left_side()
        across(0)
        right_side()

    pl.when(gx > 1)(lambda: across(1))


    with scope("z_wait"):
        group_arrived(Z)
    with scope("around"):
        for r in row_blocks:
            assemble(r)
        for t in range(STEPS):
            for r in blocks_of(t):
                around(t, r)
        for x in range(cells_x):
            for r in final_blocks:
                rows = pl.ds(r - TOP, TILE)
                values = merged(x, r, [out_ref[c, x, rows, :] for c in range(comps)])
                for c in range(comps):
                    out_ref[c, x, rows, :] = values[c]

    def finish(dy):
        r = low_rows if dy > 0 else high_rows
        with scope("y_wait%d" % dy):
            y_arrived(dy)
        with scope("win%d" % dy):
            ghosts(r)
            end_ghost(r)
            assemble(r)
            for t in range(STEPS):
                beyond = STEPS - 1 - t
                around(t, r)
                planes(t, -beyond, cells_x + beyond, [r])

    @pl.when(bottom)
    def _():
        finish(-1)
        finish(1)

    @pl.when(~bottom)
    def _():
        finish(1)
        finish(-1)

    with scope("drain"):
        total = {dx: sum(rows for (_, d), rows in volume.items() if d == dx)
                 for dx in (-1, 0, 1)}
        settle_by_place(send_sem.at[0], total[-1], total[0], total[1])
        fed = cells_y + 2 * reach
        whole = lax.div(gx, share) == gz
        pl.when(~at_left & whole)(lambda: settle(send_sem.at[1], feed_planes * fed))
        pl.when(~at_left & (share - gz == gx))(lambda: settle(send_sem.at[1], fed))
        pl.when(at_left & whole)(lambda: settle(send_sem.at[1], 2 * feed_planes * reach))
        if share == 1:
            pl.when(at_left & (gz == 1))(lambda: settle(send_sem.at[1], 2 * reach))


def local(sizes, velocity, plane_early, plane_late, blend):
    comps, cells_x, cells_y, cells_z = velocity.shape
    nx, ny, nz = sizes
    groups = cells_z // GROUP
    assert nz == 2 and ny > 2 and nx % nz == 0 and cells_z == 128
    assert cells_x == 2 * groups and 2 * DEPTH == groups and cells_y % TILE == 0
    assert TILE == 2 * DEPTH and comps <= groups
    share = nx // nz
    feed_planes = -(-comps // share)
    assert plane_early.shape[2] * share == cells_z
    dma = pltpu.SemaphoreType.DMA
    padded = cells_y + 2 * TOP
    planes = cells_x + 2 * DEPTH
    return pl.pallas_call(
        functools.partial(kernel, sizes),
        out_shape=pltpu.VMEM(velocity.shape, velocity.dtype),
        in_specs=[pl.BlockSpec(memory_space=pl.ANY)] * 3
        + [pl.BlockSpec(memory_space=pltpu.SMEM)],
        out_specs=pl.BlockSpec(memory_space=pltpu.VMEM),
        scratch_shapes=[
            pltpu.VMEM((STEPS + 1, comps, planes + 3, padded, cells_z), jnp.float32),
            pltpu.VMEM((comps + 2, cells_y, cells_z), jnp.float32),
            pltpu.VMEM((comps + 2, padded, cells_z), jnp.float32),
            pltpu.VMEM((feed_planes + 1, cells_y, cells_z), jnp.float32),
            pltpu.VMEM((nx, feed_planes + 1, padded, cells_z), jnp.float32),
            pltpu.VMEM((comps, padded, cells_z), jnp.float32),
            pltpu.VMEM((comps, padded, cells_z), jnp.float32),
            pltpu.VMEM(plane_early.shape, jnp.float32),
            pltpu.VMEM(plane_late.shape, jnp.float32),
            pltpu.VMEM((2 * comps * planes * padded, cells_z), jnp.float32),
            pltpu.SemaphoreType.REGULAR((3,)), dma((3,)), dma((2,)), dma((6,)),
        ],
        compiler_params=pltpu.CompilerParams(collective_id=0, has_side_effects=True),
        name="advect_substeps",
    )(velocity, plane_early, plane_late, blend)


def solution(mesh):
    sizes = tuple(mesh.shape[name] for name in ("gx", "gy", "gz"))
    return jax.shard_map(
        functools.partial(local, sizes),
        mesh=mesh,
        in_specs=(P(None, "gx", "gy", "gz"), P(None, "gy", "gx"), P(None, "gy", "gx"), P()),
        out_specs=P(None, "gx", "gy", "gz"),
        check_vma=False,
    )
```
